8 devices in a mesh: dp: 1 (over z), row: 2 (over y), co: 2 (over x), ci: 2 (over core).
Axes of the slice: x: 2, y: 2, z: 1, core: 2. Of those that a mesh axis runs over, the one named last changes fastest.
Arguments:
- x_in: bfloat16 [4096, 4096], P(('dp', 'row'), ('co', 'ci'))
- w_up: bfloat16 [4096, 14336], P('row', ('co', 'ci'))
- w_down: bfloat16 [14336, 4096], P('row', ('co', 'ci'))
Outputs:
- output: bfloat16 [4096, 4096], P(('dp', 'row'), ('co', 'ci'))
All inputs are finite; a program needn't handle non-finite values.
Results may differ from the reference program's by a relative error of at most 0.001.
Values are sent between devices in bfloat16 or wider.
A program may use at most 1 GiB of HBM per device.

```python
import jax
import jax.numpy as jnp
from jax import lax

TOK_DEV = 2048
D = 4096
F = 14336
ROW_GROUPS = 2


def setup_inputs(seed: int = 0, part: int = 0) -> dict:
    root_key = jax.random.key(seed)
    key_x = jax.random.fold_in(jax.random.fold_in(root_key, 1), part)
    key_up = jax.random.fold_in(root_key, 2)
    key_down = jax.random.fold_in(root_key, 3)
    x_in = jax.random.normal(key_x, (ROW_GROUPS * TOK_DEV, D), jnp.float32)
    w_up = jax.random.normal(key_up, (D, F), jnp.float32) * (D ** -0.5)
    w_down = jax.random.normal(key_down, (F, D), jnp.float32) * (F ** -0.5)
    return {"x_in": x_in.astype(jnp.bfloat16), "w_up": w_up.astype(jnp.bfloat16), "w_down": w_down.astype(jnp.bfloat16)}


def reference(x_in, w_up, w_down):
    x_blocks = x_in.reshape(ROW_GROUPS, TOK_DEV, D)

    def row_block(x_rows):
        pre_act = jnp.dot(x_rows, w_up, preferred_element_type=jnp.float32)
        hidden = jax.nn.gelu(pre_act, approximate=True).astype(jnp.bfloat16)
        return jnp.dot(hidden, w_down, preferred_element_type=jnp.float32).astype(jnp.bfloat16)

    y_blocks = lax.map(row_block, x_blocks)
    return y_blocks.reshape(ROW_GROUPS * TOK_DEV, D)
```

```python
import jax
import jax.numpy as jnp
from jax import lax
from jax.sharding import PartitionSpec as P

ROW_AXES = ("dp", "row")
COL_AXES = ("co", "ci")
SWAP = [(0, 1), (1, 0)]
NUP = 4
NDN = 8


def solution(mesh):
    def local_mlp(x, w1, w2):
        row, co, ci = lax.axis_index("row"), lax.axis_index("co"), lax.axis_index("ci")
        f32 = jnp.float32
        fq = w1.shape[1] // NUP
        w1c = [w1[:, i * fq:(i + 1) * fq] for i in range(NUP)]
        w1p = [lax.ppermute(c, "row", SWAP) for c in w1c]
        fd = w2.shape[0] // NDN
        w2c = [w2[i * fd:(i + 1) * fd] for i in range(NDN)]
        w2p = [lax.ppermute(c, "row", SWAP) for c in w2c]

        def by_core(own, mate):
            first = ci == 0
            return jnp.concatenate([jnp.where(first, own, mate), jnp.where(first, mate, own)], axis=1)

        def gather(blk):
            far = lax.ppermute(blk, "co", SWAP)
            mate = lax.ppermute(blk, "ci", SWAP)
            far_mate = lax.ppermute(far, "ci", SWAP)
            here, there = (blk, mate), (far, far_mate)
            same = co == row
            pick = lambda a, b: jnp.where(same, a, b)
            near = [pick(a, b) for a, b in zip(here, there)]
            away = [pick(b, a) for a, b in zip(here, there)]
            first = ci == 0
            order = lambda p: [jnp.where(first, p[0], p[1]), jnp.where(first, p[1], p[0])]
            return order(near), order(away)

        xn, xa = gather(x)
        x_near = jnp.concatenate(xn, axis=1)
        x_away = jnp.concatenate(xa, axis=1)
        hn, ha = [], []
        for i in range(NUP):
            pre = jnp.dot(x_near, w1c[i], preferred_element_type=f32) + jnp.dot(x_away, w1p[i], preferred_element_type=f32)
            h = jax.nn.gelu(pre, approximate=True).astype(jnp.bfloat16)
            n, a = gather(h)
            hn.append(n)
            ha.append(a)
        acc = None
        half = w2.shape[0] // 2
        for i in range(NUP):
            for k in range(2):
                t = jnp.dot(hn[i][k], w2[k * half + i * fq:k * half + (i + 1) * fq], preferred_element_type=f32)
                acc = t if acc is None else acc + t
        for j in range(NDN):
            k, i = divmod(j, NUP)
            acc = acc + jnp.dot(ha[i][k], w2p[j], preferred_element_type=f32)
        return acc.astype(jnp.bfloat16)

    act_spec = P(ROW_AXES, COL_AXES)
    wgt_spec = P("row", COL_AXES)
    return jax.shard_map(local_mlp, mesh=mesh, in_specs=(act_spec, wgt_spec, wgt_spec), out_specs=act_spec, check_vma=False)
```

```python
import functools
import math

import jax
import jax.numpy as jnp
from jax import lax
from jax.experimental import pallas as pl
from jax.experimental.pallas import tpu as pltpu
from jax.sharding import PartitionSpec as P

ROW_AXES = ("dp", "row")
COL_AXES = ("co", "ci")
MESH = pl.DeviceIdType.MESH
FC = 512
TM = 256
GELU_C = math.sqrt(2.0 / math.pi)


def gelu(p):
    return 0.5 * p * (1.0 + jnp.tanh(GELU_C * (p + 0.044715 * (p * p * p))))


def kernel(x, w1, w2, y, w1p, hq, xv, wv, hv, hb, wb, w2p, acc, yv,
           s_w1, r_w1, s_w2, r_w2, s_x, r_x, s_hfar, r_hfar, s_hmate, r_hmate, s_fwd, r_fwd,
           s_hloc, s_ld, s_hb, s_wb, s_y):
    f32 = jnp.float32
    rows, kq = x.shape
    kh, fq = w1.shape
    n_up = fq // FC
    n_dn = w2.shape[0] // FC
    row, co, ci = lax.axis_index("row"), lax.axis_index("co"), lax.axis_index("ci")
    vert, far, mate = {"row": 1 - row}, {"co": 1 - co}, {"ci": 1 - ci}

    barrier = pltpu.get_barrier_semaphore()
    for dev in (vert, far, mate):
        pl.semaphore_signal(barrier, inc=1, device_id=dev, device_id_type=MESH)
    pl.semaphore_wait(barrier, 3)

    def rdma(src, dst, send, recv, dev):
        return pltpu.make_async_remote_copy(
            src_ref=src, dst_ref=dst, send_sem=send, recv_sem=recv, device_id=dev, device_id_type=MESH)

    def cols(i):
        return pl.ds(pl.multiple_of(i * FC, FC), FC)

    def w1_copy(i):
        return rdma(w1.at[:, cols(i)], w1p.at[:, cols(i)], s_w1.at[i], r_w1.at[i], vert)

    def w2_copy(i):
        return rdma(w2.at[cols(i)], w2p.at[cols(i)], s_w2.at[i], r_w2.at[i], vert)

    x_far = rdma(x, xv.at[co, ci], s_x.at[0], r_x.at[0], far)
    x_mate = rdma(x, xv.at[co, ci], s_x.at[1], r_x.at[1], mate)
    x_fwd = rdma(xv.at[1 - co, ci], xv.at[1 - co, ci], s_x.at[2], r_x.at[2], mate)
    x_own = pltpu.make_async_copy(x, xv.at[co, ci], s_ld.at[0])

    def start(copy):
        def body(i, c):
            copy(i).start()
            return c
        return body

    w1_copy(0).start()
    x_far.start()
    x_mate.start()
    x_own.start()
    lax.fori_loop(1, n_up, start(w1_copy), 0)
    lax.fori_loop(0, n_dn, start(w2_copy), 0)
    x_own.wait()
    x_mate.wait()
    x_far.wait()
    x_fwd.start()
    x_fwd.wait()

    def h_copies(i, slot):
        src = hv.at[slot]
        dst = hq.at[co, ci, :, cols(i)]
        return (rdma(src, dst, s_hfar.at[i], r_hfar.at[i], far),
                rdma(src, dst, s_hmate.at[i], r_hmate.at[i], mate),
                pltpu.make_async_copy(src, dst, s_hloc.at[slot]))

    def h_forward(i):
        blk = hq.at[1 - co, ci, :, cols(i)]
        return rdma(blk, blk, s_fwd.at[i], r_fwd.at[i], mate)

    def h_drain(i, slot):
        a, b, c = h_copies(i, slot)
        a.wait_send()
        b.wait_send()
        c.wait()

    def up(i, carry):
        slot = lax.rem(i, 2)
        own = pltpu.make_async_copy(w1.at[:, cols(i)], wv.at[row], s_ld.at[0])
        own.start()
        w1_copy(i).wait_recv()
        peer = pltpu.make_async_copy(w1p.at[:, cols(i)], wv.at[1 - row], s_ld.at[1])
        peer.start()

        @pl.when(i >= 2)
        def _():
            h_drain(i - 2, slot)
            a, _, _ = h_copies(i - 2, slot)
            a.wait_recv()
            h_forward(i - 2).start()

        own.wait()
        peer.wait()

        def tile(m, c):
            r = pl.ds(pl.multiple_of(m * TM, TM), TM)
            p = None
            for k in range(4):
                a, b = divmod(k, 2)
                t = jnp.dot(xv[a, b, r, :], wv[a, b * kq:(b + 1) * kq, :], preferred_element_type=f32)
                p = t if p is None else p + t
            hv[slot, r, :] = gelu(p).astype(jnp.bfloat16)
            return c

        lax.fori_loop(0, rows // TM, tile, 0)
        for c in h_copies(i, slot):
            c.start()
        return carry

    lax.fori_loop(0, n_up, up, 0)

    def tail(i, carry):
        slot = lax.rem(i, 2)
        h_drain(i, slot)
        a, _, _ = h_copies(i, slot)
        a.wait_recv()
        h_forward(i).start()
        return carry

    lax.fori_loop(n_up - 2, n_up, tail, 0)

    def settle(i, carry):
        _, b, _ = h_copies(i, lax.rem(i, 2))
        b.wait_recv()
        h_forward(i).wait()
        return carry

    lax.fori_loop(0, n_up, settle, 0)

    def h_load(t, side):
        return pltpu.make_async_copy(
            hq.at[side, t // n_up, :, cols(lax.rem(t, n_up))], hb.at[lax.rem(t, 2)], s_hb.at[lax.rem(t, 2)])

    def w2_load(t):
        return pltpu.make_async_copy(w2.at[cols(t)], wb.at[lax.rem(t, 2)], s_wb.at[lax.rem(t, 2)])

    acc[...] = jnp.zeros_like(acc)
    h_load(0, row).start()
    w2_load(0).start()

    def near(t, carry):
        slot = lax.rem(t, 2)

        @pl.when(t + 1 < n_dn)
        def _():
            h_load(t + 1, row).start()
            w2_load(t + 1).start()

        h_load(t, row).wait()
        w2_load(t).wait()

        def tile(m, c):
            r = pl.ds(pl.multiple_of(m * TM, TM), TM)
            acc[r, :] += jnp.dot(hb[slot, r, :], wb[slot], preferred_element_type=f32)
            return c

        lax.fori_loop(0, rows // TM, tile, 0)
        return carry

    lax.fori_loop(0, n_dn, near, 0)
    h_load(0, 1 - row).start()

    def away(t, carry):
        slot = lax.rem(t, 2)
        h_load(t + 1, 1 - row).start()
        h_load(t, 1 - row).wait()
        w2_copy(t).wait_recv()

        def tile(m, c):
            r = pl.ds(pl.multiple_of(m * TM, TM), TM)
            acc[r, :] += jnp.dot(hb[slot, r, :], w2p[cols(t), :], preferred_element_type=f32)
            return c

        lax.fori_loop(0, rows // TM, tile, 0)
        return carry

    lax.fori_loop(0, n_dn - 1, away, 0)

    t = n_dn - 1
    slot = t % 2
    h_load(t, 1 - row).wait()
    w2_copy(t).wait_recv()

    def y_copy(m):
        r = pl.ds(pl.multiple_of(m * TM, TM), TM)
        return pltpu.make_async_copy(yv.at[r], y.at[r], s_y.at[m])

    def last(m, c):
        r = pl.ds(pl.multiple_of(m * TM, TM), TM)
        out = acc[r, :] + jnp.dot(hb[slot, r, :], w2p[t * FC:(t + 1) * FC, :], preferred_element_type=f32)
        yv[r, :] = out.astype(jnp.bfloat16)
        y_copy(m).start()
        return c

    lax.fori_loop(0, rows // TM, last, 0)

    def w1_sent(i, c):
        w1_copy(i).wait_send()
        return c

    def w2_sent(i, c):
        w2_copy(i).wait_send()
        return c

    lax.fori_loop(0, n_up, w1_sent, 0)
    lax.fori_loop(0, n_dn, w2_sent, 0)

    def y_done(m, c):
        y_copy(m).wait()
        return c

    lax.fori_loop(0, rows // TM, y_done, 0)


def solution(mesh):
    def local_mlp(x, w1, w2):
        rows, kq = x.shape
        kh, fq = w1.shape
        fh, nq = w2.shape
        n_up, n_dn = fq // FC, fh // FC
        bf, f32 = jnp.bfloat16, jnp.float32
        hbm = pl.BlockSpec(memory_space=pltpu.HBM)
        dma = lambda n: pltpu.SemaphoreType.DMA((n,))
        outs = pl.pallas_call(
            kernel,
            name="mlp",
            out_shape=(
                jax.ShapeDtypeStruct((rows, nq), bf),
                jax.ShapeDtypeStruct((kh, fq), bf),
                jax.ShapeDtypeStruct((2, 2, rows, fq), bf),
            ),
            in_specs=[hbm] * 3,
            out_specs=(hbm,) * 3,
            scratch_shapes=[
                pltpu.VMEM((2, 2, rows, kq), bf),
                pltpu.VMEM((2, kh, FC), bf),
                pltpu.VMEM((2, rows, FC), bf),
                pltpu.VMEM((2, rows, FC), bf),
                pltpu.VMEM((2, FC, nq), bf),
                pltpu.VMEM((fh, nq), bf),
                pltpu.VMEM((rows, nq), f32),
                pltpu.VMEM((rows, nq), bf),
                dma(n_up), dma(n_up), dma(n_dn), dma(n_dn), dma(3), dma(3),
                dma(n_up), dma(n_up), dma(n_up), dma(n_up), dma(n_up), dma(n_up),
                dma(2), dma(2), dma(2), dma(2), dma(rows // TM),
            ],
            compiler_params=pltpu.CompilerParams(
                collective_id=0, has_side_effects=True, vmem_limit_bytes=67_000_000),
        )(x, w1, w2)
        return outs[0]

    act_spec = P(ROW_AXES, COL_AXES)
    wgt_spec = P("row", COL_AXES)
    return jax.shard_map(local_mlp, mesh=mesh, in_specs=(act_spec, wgt_spec, wgt_spec), out_specs=act_spec, check_vma=False)
```

```python
import math

import jax
import jax.numpy as jnp
from jax import lax
from jax.experimental import pallas as pl
from jax.experimental.pallas import tpu as pltpu
from jax.sharding import PartitionSpec as P

ROW_AXES = ("dp", "row")
COL_AXES = ("co", "ci")
MESH = pl.DeviceIdType.MESH
T = 256
TN = 256
LAG_FWD = 2
LAG_DOWN = 3
SLOTS = 4
GELU_C = math.sqrt(2.0 / math.pi)


def gelu(p):
    return 0.5 * p * (1.0 + jnp.tanh(GELU_C * (p + 0.044715 * (p * p * p))))


def each(lo, hi, fn):
    def body(i, c):
        fn(i)
        return c

    lax.fori_loop(lo, hi, body, 0)


def kernel(x, w1, w2, y, xg, hg, yp, wv, w2v, xv, hv, hb, yf, yin, yo,
           s_xa, r_xa, s_xb, r_xb, s_xc, r_xc, s_xd, r_xd, s_xe, r_xe, s_xf, r_xf, s_xh, r_xh,
           s_w, r_w, s_l, s_hl, s_hf, r_hf, s_hm, r_hm, s_hw, r_hw, s_yf, r_yf, s_ld, s_yo):
    f32 = jnp.float32
    rows, kq = x.shape
    kh, fq = w1.shape
    nq = w2.shape[1]
    hc = fq // 2
    n = rows // T
    steps = 2 * n
    row, co, ci = lax.axis_index("row"), lax.axis_index("co"), lax.axis_index("ci")
    vert, far, mate = {"row": 1 - row}, {"co": 1 - co}, {"ci": 1 - ci}
    corner = {"row": 1 - row, "co": 1 - co}

    barrier = pltpu.get_barrier_semaphore()
    for dev in (vert, far, mate, corner):
        pl.semaphore_signal(barrier, inc=1, device_id=dev, device_id_type=MESH)
    pl.semaphore_wait(barrier, 4)

    def rdma(src, dst, send, recv, dev):
        return pltpu.make_async_remote_copy(
            src_ref=src, dst_ref=dst, send_sem=send, recv_sem=recv, device_id=dev, device_id_type=MESH)

    def tok(j):
        return pl.ds(pl.multiple_of(j * T, T), T)

    def half(c):
        return pl.ds(pl.multiple_of(c * hc, TN), hc)

    def xa(j):
        return rdma(x.at[tok(j)], xg.at[row, co, ci, tok(j)], s_xa.at[j], r_xa.at[j], far)

    def xb(j):
        return rdma(x.at[tok(j)], xg.at[row, co, ci, tok(j)], s_xb.at[j], r_xb.at[j], vert)

    def pass_on(r, c, j, send, recv, dev):
        blk = xg.at[r, c, ci, tok(j)]
        return rdma(blk, blk, send.at[j], recv.at[j], dev)

    def xc(j):
        return pass_on(row, 1 - co, j, s_xc, r_xc, vert)

    def xe(j):
        return pass_on(row, 1 - co, j, s_xe, r_xe, mate)

    def xf(j):
        return pass_on(1 - row, co, j, s_xf, r_xf, mate)

    def xh(j):
        return pass_on(1 - row, 1 - co, j, s_xh, r_xh, mate)

    xd = rdma(x, xg.at[row, co, ci], s_xd.at[0], r_xd.at[0], mate)

    w_x = rdma(w1.at[:, half(1 - co)], wv.at[row], s_w.at[0], r_w.at[row], {"row": co, "co": 1 - co})

    def w_y():
        return rdma(w1.at[:, half(co)], wv.at[row], s_w.at[1], r_w.at[row], vert)

    def w_here():
        return pltpu.make_async_copy(w1.at[:, half(co)], wv.at[row], s_l.at[0])

    def w_in(k):
        return rdma(w1.at[:, half(0)], wv.at[k], s_w.at[1], r_w.at[k], vert)

    w2_in = pltpu.make_async_copy(w2, w2v, s_l.at[1])

    def hf(i):
        return rdma(hv.at[lax.rem(i, SLOTS)], hg.at[co, ci, tok(i)], s_hf.at[i], r_hf.at[i], far)

    def hm(i):
        return rdma(hv.at[lax.rem(i, SLOTS)], hg.at[co, ci, tok(i)], s_hm.at[i], r_hm.at[i], mate)

    def hl(i):
        s = lax.rem(i, SLOTS)
        return pltpu.make_async_copy(hv.at[s], hg.at[co, ci, tok(i)], s_hl.at[s])

    def hw(i):
        blk = hg.at[1 - co, ci, tok(i)]
        return rdma(blk, blk, s_hw.at[i], r_hw.at[i], mate)

    def yc(j):
        return rdma(yf.at[j], yp.at[tok(j)], s_yf.at[j], r_yf.at[j], vert)

    def y_out(j):
        s = lax.rem(j, 2)
        return pltpu.make_async_copy(yo.at[s], y.at[tok(j)], s_yo.at[s])

    def relay(j):
        xc(j).start()
        xe(j).start()

    def meet(j):
        xb(j).wait_recv()
        xc(j).wait_recv()
        xf(j).start()
        xh(j).start()

    each(0, 2, lambda j: xa(j).start())
    each(0, 2, lambda j: xb(j).start())
    w_x.start()
    each(2, n, lambda j: xa(j).start())
    xd.start()
    w2_in.start()

    @pl.when(row == co)
    def _():
        w_here().start()

    def first(j):
        xa(j).wait_recv()
        relay(j)

    each(0, 2, first)

    @pl.when(row != co)
    def _():
        w_y().start()

    meet(0)

    @pl.when(row == co)
    def _():
        w_here().wait()
        w_in(1 - row).wait_recv()

    @pl.when(row != co)
    def _():
        w_in(0).wait_recv()
        w_in(1).wait_recv()

    w2_in.wait()

    def up(k):
        @pl.when(k < n)
        def _():
            xf(k).wait_recv()
            xh(k).wait_recv()
            ld = pltpu.make_async_copy(xg.at[1 - row, :, :, tok(k)], xv, s_ld.at[0])
            ld.start()
            ld.wait()

        @pl.when(k == n)
        def _():
            xd.wait_recv()

        @pl.when(k >= n)
        def _():
            j = k - n
            xe(j).wait_recv()
            lds = (
                pltpu.make_async_copy(xg.at[row, 1 - co, :, tok(j)], xv.at[1 - co], s_ld.at[0]),
                pltpu.make_async_copy(xg.at[row, co, 1 - ci, tok(j)], xv.at[co, 1 - ci], s_ld.at[1]),
                pltpu.make_async_copy(x.at[tok(j)], xv.at[co, ci], s_ld.at[2]),
            )
            for c in lds:
                c.start()
            for c in lds:
                c.wait()

        @pl.when(k >= SLOTS)
        def _():
            hf(k - SLOTS).wait_send()
            hm(k - SLOTS).wait_send()

        s = lax.rem(k, SLOTS)

        def tile(t):
            cols = pl.ds(pl.multiple_of(t * TN, TN), TN)
            p = None
            for a in range(2):
                for b in range(2):
                    d = jnp.dot(xv[a, b], wv[a, b * kq:(b + 1) * kq, cols], preferred_element_type=f32)
                    p = d if p is None else p + d
            hv[s, :, cols] = gelu(p).astype(jnp.bfloat16)

        each(0, hc // TN, tile)
        hf(k).start()
        hm(k).start()
        hl(k).start()

    def down(i):
        hl(i).wait()
        hm(i).wait_recv()
        hw(i).wait_recv()
        ld = pltpu.make_async_copy(hg.at[:, :, tok(i)], hb, s_ld.at[3])
        ld.start()
        other = i < n
        j = jnp.where(other, i, i - n)
        s = jnp.where(other, i, n)

        @pl.when(jnp.logical_not(other))
        def _():
            yc(j).wait_recv()
            part = pltpu.make_async_copy(yp.at[tok(j)], yin, s_ld.at[4])
            part.start()
            part.wait()

        ld.wait()

        def tile(t):
            cols = pl.ds(pl.multiple_of(t * TN, TN), TN)
            p = None
            for b in range(2):
                for a in range(2):
                    lo = b * fq + a * hc
                    d = jnp.dot(hb[a, b], w2v[lo:lo + hc, cols], preferred_element_type=f32)
                    p = d if p is None else p + d
            yf[s, :, cols] = p

        each(0, nq // TN, tile)

        @pl.when(other)
        def _():
            yc(j).start()

        @pl.when(jnp.logical_not(other))
        def _():
            @pl.when(j >= 2)
            def _():
                y_out(j - 2).wait()

            yo[lax.rem(j, 2)] = (yf[n] + yin[...]).astype(jnp.bfloat16)
            y_out(j).start()

    def step(k):
        @pl.when(k < steps)
        def _():
            up(k)

        @pl.when(k + 2 < n)
        def _():
            xa(k + 2).wait_recv()
            xb(k + 2).start()
            relay(k + 2)

        @pl.when(k + 1 < n)
        def _():
            meet(k + 1)

        @pl.when((k >= LAG_FWD) & (k < steps + LAG_FWD))
        def _():
            hf(k - LAG_FWD).wait_recv()
            hw(k - LAG_FWD).start()

        @pl.when(k >= LAG_DOWN)
        def _():
            down(k - LAG_DOWN)

    each(0, steps + LAG_DOWN, step)

    w_x.wait_send()

    @pl.when(row != co)
    def _():
        w_y().wait_send()

    xd.wait_send()

    def sent_x(j):
        for c in (xa, xb, xc, xe, xf, xh, yc):
            c(j).wait_send()

    each(0, n, sent_x)
    each(0, steps, lambda i: hw(i).wait_send())

    def sent_h(i):
        hf(i).wait_send()
        hm(i).wait_send()

    each(steps - SLOTS, steps, sent_h)
    each(n - 2, n, lambda j: y_out(j).wait())


def solution(mesh):
    def local_mlp(x, w1, w2):
        rows, kq = x.shape
        kh, fq = w1.shape
        fh, nq = w2.shape
        hc, n = fq // 2, rows // T
        bf, f32 = jnp.bfloat16, jnp.float32
        hbm = pl.BlockSpec(memory_space=pltpu.HBM)
        dma = lambda k: pltpu.SemaphoreType.DMA((k,))
        outs = pl.pallas_call(
            kernel,
            name="mlp",
            out_shape=(
                jax.ShapeDtypeStruct((rows, nq), bf),
                jax.ShapeDtypeStruct((2, 2, 2, rows, kq), bf),
                jax.ShapeDtypeStruct((2, 2, 2 * rows, hc), bf),
                jax.ShapeDtypeStruct((rows, nq), f32),
            ),
            in_specs=[hbm] * 3,
            out_specs=(hbm,) * 4,
            scratch_shapes=[
                pltpu.VMEM((2, kh, hc), bf),
                pltpu.VMEM((fh, nq), bf),
                pltpu.VMEM((2, 2, T, kq), bf),
                pltpu.VMEM((SLOTS, T, hc), bf),
                pltpu.VMEM((2, 2, T, hc), bf),
                pltpu.VMEM((n + 1, T, nq), f32),
                pltpu.VMEM((T, nq), f32),
                pltpu.VMEM((2, T, nq), bf),
                dma(n), dma(n), dma(n), dma(n), dma(n), dma(n), dma(1), dma(1),
                dma(n), dma(n), dma(n), dma(n), dma(n), dma(n),
                dma(2), dma(2), dma(2), dma(SLOTS),
                dma(2 * n), dma(2 * n), dma(2 * n), dma(2 * n), dma(2 * n), dma(2 * n),
                dma(n), dma(n), dma(5), dma(2),
            ],
            compiler_params=pltpu.CompilerParams(
                collective_id=0, has_side_effects=True, vmem_limit_bytes=67_000_000),
        )(x, w1, w2)
        return outs[0]

    act_spec = P(ROW_AXES, COL_AXES)
    wgt_spec = P("row", COL_AXES)
    return jax.shard_map(local_mlp, mesh=mesh, in_specs=(act_spec, wgt_spec, wgt_spec), out_specs=act_spec, check_vma=False)
```

```python
import math

import jax
import jax.numpy as jnp
from jax import lax
from jax.experimental import pallas as pl
from jax.experimental.pallas import tpu as pltpu
from jax.sharding import PartitionSpec as P

ROW_AXES = ("dp", "row")
COL_AXES = ("co", "ci")
MESH = pl.DeviceIdType.MESH
T = 256
TN = 256
LAG_FWD = 2
LAG_DOWN = 3
SLOTS = 4
GELU_C = math.sqrt(2.0 / math.pi)


def gelu(p):
    return 0.5 * p * (1.0 + jnp.tanh(GELU_C * (p + 0.044715 * (p * p * p))))


def each(lo, hi, fn):
    def body(i, c):
        fn(i)
        return c

    lax.fori_loop(lo, hi, body, 0)


def kernel(x, w1, w2, y, xg, hg, yp, wv, w2v, xv, hv, hb, yf, yin, yo,
           s_xa, r_xa, s_xb, r_xb, s_xc, r_xc, s_xd, r_xd, s_xe, r_xe, s_xf, r_xf, s_xh, r_xh,
           s_w, r_w, s_l, s_hl, s_hf, r_hf, s_hm, r_hm, s_hw, r_hw, s_yf, r_yf, s_ld, s_yo):
    f32 = jnp.float32
    rows, kq = x.shape
    kh, fq = w1.shape
    nq = w2.shape[1]
    hc = fq // 2
    n = rows // T
    steps = 2 * n
    row, co, ci = lax.axis_index("row"), lax.axis_index("co"), lax.axis_index("ci")
    vert, far, mate = {"row": 1 - row}, {"co": 1 - co}, {"ci": 1 - ci}
    corner = {"row": 1 - row, "co": 1 - co}

    barrier = pltpu.get_barrier_semaphore()
    for dev in (vert, far, mate, corner):
        pl.semaphore_signal(barrier, inc=1, device_id=dev, device_id_type=MESH)
    pl.semaphore_wait(barrier, 4)

    def rdma(src, dst, send, recv, dev):
        return pltpu.make_async_remote_copy(
            src_ref=src, dst_ref=dst, send_sem=send, recv_sem=recv, device_id=dev, device_id_type=MESH)

    def tok(j):
        return pl.ds(pl.multiple_of(j * T, T), T)

    def half(c):
        return pl.ds(pl.multiple_of(c * hc, TN), hc)

    def xa(j):
        return rdma(x.at[tok(j)], xg.at[row, co, ci, tok(j)], s_xa.at[j], r_xa.at[j], far)

    def xb(j):
        return rdma(x.at[tok(j)], xg.at[row, co, ci, tok(j)], s_xb.at[j], r_xb.at[j], vert)

    def pass_on(r, c, j, send, recv, dev):
        blk = xg.at[r, c, ci, tok(j)]
        return rdma(blk, blk, send.at[j], recv.at[j], dev)

    def xc(j):
        return pass_on(row, 1 - co, j, s_xc, r_xc, vert)

    def xe(j):
        return pass_on(row, 1 - co, j, s_xe, r_xe, mate)

    def xf(j):
        return pass_on(1 - row, co, j, s_xf, r_xf, mate)

    def xh(j):
        return pass_on(1 - row, 1 - co, j, s_xh, r_xh, mate)

    xd = rdma(x, xg.at[row, co, ci], s_xd.at[0], r_xd.at[0], mate)

    w_x = rdma(w1.at[:, half(1 - co)], wv.at[row], s_w.at[0], r_w.at[row], {"row": co, "co": 1 - co})

    def w_y():
        return rdma(w1.at[:, half(co)], wv.at[row], s_w.at[1], r_w.at[row], vert)

    def w_here():
        return pltpu.make_async_copy(w1.at[:, half(co)], wv.at[row], s_l.at[0])

    def w_in(k):
        return rdma(w1.at[:, half(0)], wv.at[k], s_w.at[1], r_w.at[k], vert)

    w2_in = pltpu.make_async_copy(w2, w2v, s_l.at[1])

    def hf(i):
        return rdma(hv.at[lax.rem(i, SLOTS)], hg.at[co, ci, tok(i)], s_hf.at[i], r_hf.at[i], far)

    def hm(i):
        return rdma(hv.at[lax.rem(i, SLOTS)], hg.at[co, ci, tok(i)], s_hm.at[i], r_hm.at[i], mate)

    def hl(i):
        s = lax.rem(i, SLOTS)
        return pltpu.make_async_copy(hv.at[s], hg.at[co, ci, tok(i)], s_hl.at[s])

    def hw(i):
        blk = hg.at[1 - co, ci, tok(i)]
        return rdma(blk, blk, s_hw.at[i], r_hw.at[i], mate)

    def yc(j):
        return rdma(yf.at[j], yp.at[tok(j)], s_yf.at[j], r_yf.at[j], vert)

    def y_out(j):
        s = lax.rem(j, 2)
        return pltpu.make_async_copy(yo.at[s], y.at[tok(j)], s_yo.at[s])

    def relay(j):
        xc(j).start()
        xe(j).start()

    def meet(j):
        xb(j).wait_recv()
        xc(j).wait_recv()
        xf(j).start()
        xh(j).start()

    each(0, 2, lambda j: xa(j).start())
    each(0, 2, lambda j: xb(j).start())
    w_x.start()
    each(2, n, lambda j: xa(j).start())
    xd.start()
    w2_in.start()

    @pl.when(row == co)
    def _():
        w_here().start()

    def first(j):
        xa(j).wait_recv()
        relay(j)

    each(0, 2, first)

    @pl.when(row != co)
    def _():
        w_y().start()

    meet(0)

    @pl.when(row == co)
    def _():
        w_here().wait()
        w_in(1 - row).wait_recv()

    @pl.when(row != co)
    def _():
        w_in(0).wait_recv()
        w_in(1).wait_recv()

    w2_in.wait()

    def up(k):
        @pl.when(k < n)
        def _():
            xf(k).wait_recv()
            xh(k).wait_recv()
            ld = pltpu.make_async_copy(xg.at[1 - row, :, :, tok(k)], xv, s_ld.at[0])
            ld.start()
            ld.wait()

        @pl.when(k == n)
        def _():
            xd.wait_recv()

        @pl.when(k >= n)
        def _():
            j = k - n
            xe(j).wait_recv()
            lds = (
                pltpu.make_async_copy(xg.at[row, 1 - co, :, tok(j)], xv.at[1 - co], s_ld.at[0]),
                pltpu.make_async_copy(xg.at[row, co, 1 - ci, tok(j)], xv.at[co, 1 - ci], s_ld.at[1]),
                pltpu.make_async_copy(x.at[tok(j)], xv.at[co, ci], s_ld.at[2]),
            )
            for c in lds:
                c.start()
            for c in lds:
                c.wait()

        @pl.when(k >= SLOTS)
        def _():
            hf(k - SLOTS).wait_send()
            hm(k - SLOTS).wait_send()

        s = lax.rem(k, SLOTS)

        def tile(t):
            cols = pl.ds(pl.multiple_of(t * TN, TN), TN)
            p = None
            for a in range(2):
                for b in range(2):
                    d = jnp.dot(xv[a, b], wv[a, b * kq:(b + 1) * kq, cols], preferred_element_type=f32)
                    p = d if p is None else p + d
            hv[s, :, cols] = gelu(p).astype(jnp.bfloat16)

        each(0, hc // TN, tile)
        hf(k).start()
        hm(k).start()
        hl(k).start()

    def down(i):
        hl(i).wait()
        hm(i).wait_recv()
        hw(i).wait_recv()
        ld = pltpu.make_async_copy(hg.at[:, :, tok(i)], hb, s_ld.at[3])
        ld.start()
        other = i < n
        j = jnp.where(other, i, i - n)
        s = jnp.where(other, i, n)

        @pl.when(jnp.logical_not(other))
        def _():
            yc(j).wait_recv()
            part = pltpu.make_async_copy(yp.at[tok(j)], yin, s_ld.at[4])
            part.start()
            part.wait()

        ld.wait()

        def tile(t):
            cols = pl.ds(pl.multiple_of(t * TN, TN), TN)
            p = None
            for b in range(2):
                for a in range(2):
                    lo = b * fq + a * hc
                    d = jnp.dot(hb[a, b], w2v[lo:lo + hc, cols], preferred_element_type=f32)
                    p = d if p is None else p + d
            yf[s, :, cols] = p

        each(0, nq // TN, tile)

        @pl.when(other)
        def _():
            yc(j).start()

        @pl.when(jnp.logical_not(other))
        def _():
            @pl.when(j >= 2)
            def _():
                y_out(j - 2).wait()

            yo[lax.rem(j, 2)] = (yf[n] + yin[...]).astype(jnp.bfloat16)
            y_out(j).start()

    def bring(j):
        xa(j).wait_recv()
        xb(j).start()
        relay(j)

    def step(k):
        @pl.when(k < steps)
        def _():
            up(k)

        lo = 2 + k * (k + 1) // 2
        each(jnp.minimum(lo, n), jnp.minimum(lo + k + 1, n), bring)

        @pl.when(k + 1 < n)
        def _():
            meet(k + 1)

        @pl.when(k >= LAG_DOWN)
        def _():
            down(k - LAG_DOWN)

        @pl.when(k >= LAG_FWD)
        def _():
            hf(k - LAG_FWD).wait_recv()
            hw(k - LAG_FWD).start()

    last = steps - 1
    each(0, last + LAG_FWD, step)
    each(last - 1, last, down)

    def piece(src, dst, sem):
        c = pltpu.make_async_copy(src, dst, s_ld.at[sem])
        c.start()
        c.wait()

    def w2_rows(a, b):
        return pl.ds(pl.multiple_of(b * fq + a * hc, TN), hc)

    hl(last).wait()
    hm(last).wait_recv()
    piece(hg.at[co, :, tok(last)], hb.at[co], 0)
    yc(n - 1).wait_recv()
    piece(yp.at[tok(n - 1)], yin, 1)
    y_out(n - 3).wait()

    def near(t):
        cols = pl.ds(pl.multiple_of(t * TN, TN), TN)
        p = yin[:, cols]
        for b in range(2):
            p = p + jnp.dot(hb[co, b], w2v[w2_rows(co, b), cols], preferred_element_type=f32)
        yin[:, cols] = p

    each(0, nq // TN, near)
    hf(last).wait_recv()
    hw(last).start()
    piece(hg.at[1 - co, ci, tok(last)], hb.at[1 - co, ci], 2)

    def away(t):
        cols = pl.ds(pl.multiple_of(t * TN, TN), TN)
        yin[:, cols] += jnp.dot(hb[1 - co, ci], w2v[w2_rows(1 - co, ci), cols], preferred_element_type=f32)

    each(0, nq // TN, away)
    hw(last).wait_recv()
    piece(hg.at[1 - co, 1 - ci, tok(last)], hb.at[1 - co, 1 - ci], 3)

    def final(t):
        cols = pl.ds(pl.multiple_of(t * TN, TN), TN)
        d = jnp.dot(hb[1 - co, 1 - ci], w2v[w2_rows(1 - co, 1 - ci), cols], preferred_element_type=f32)
        yo[(n - 1) % 2, :, cols] = (yin[:, cols] + d).astype(jnp.bfloat16)

    each(0, nq // TN, final)
    y_out(n - 1).start()

    w_x.wait_send()

    @pl.when(row != co)
    def _():
        w_y().wait_send()

    xd.wait_send()

    def sent_x(j):
        for c in (xa, xb, xc, xe, xf, xh, yc):
            c(j).wait_send()

    each(0, n, sent_x)
    each(0, steps, lambda i: hw(i).wait_send())

    def sent_h(i):
        hf(i).wait_send()
        hm(i).wait_send()

    each(steps - SLOTS, steps, sent_h)
    each(n - 2, n, lambda j: y_out(j).wait())


def solution(mesh):
    def local_mlp(x, w1, w2):
        rows, kq = x.shape
        kh, fq = w1.shape
        fh, nq = w2.shape
        hc, n = fq // 2, rows // T
        bf, f32 = jnp.bfloat16, jnp.float32
        hbm = pl.BlockSpec(memory_space=pltpu.HBM)
        dma = lambda k: pltpu.SemaphoreType.DMA((k,))
        outs = pl.pallas_call(
            kernel,
            name="mlp",
            out_shape=(
                jax.ShapeDtypeStruct((rows, nq), bf),
                jax.ShapeDtypeStruct((2, 2, 2, rows, kq), bf),
                jax.ShapeDtypeStruct((2, 2, 2 * rows, hc), bf),
                jax.ShapeDtypeStruct((rows, nq), f32),
            ),
            in_specs=[hbm] * 3,
            out_specs=(hbm,) * 4,
            scratch_shapes=[
                pltpu.VMEM((2, kh, hc), bf),
                pltpu.VMEM((fh, nq), bf),
                pltpu.VMEM((2, 2, T, kq), bf),
                pltpu.VMEM((SLOTS, T, hc), bf),
                pltpu.VMEM((2, 2, T, hc), bf),
                pltpu.VMEM((n + 1, T, nq), f32),
                pltpu.VMEM((T, nq), f32),
                pltpu.VMEM((2, T, nq), bf),
                dma(n), dma(n), dma(n), dma(n), dma(n), dma(n), dma(1), dma(1),
                dma(n), dma(n), dma(n), dma(n), dma(n), dma(n),
                dma(2), dma(2), dma(2), dma(SLOTS),
                dma(2 * n), dma(2 * n), dma(2 * n), dma(2 * n), dma(2 * n), dma(2 * n),
                dma(n), dma(n), dma(5), dma(2),
            ],
            compiler_params=pltpu.CompilerParams(
                collective_id=0, has_side_effects=True, vmem_limit_bytes=67_000_000),
        )(x, w1, w2)
        return outs[0]

    act_spec = P(ROW_AXES, COL_AXES)
    wgt_spec = P("row", COL_AXES)
    return jax.shard_map(local_mlp, mesh=mesh, in_specs=(act_spec, wgt_spec, wgt_spec), out_specs=act_spec, check_vma=False)
```

```python
import math

import jax
import jax.numpy as jnp
from jax import lax
from jax.experimental import pallas as pl
from jax.experimental.pallas import tpu as pltpu
from jax.sharding import PartitionSpec as P

ROW_AXES = ("dp", "row")
COL_AXES = ("co", "ci")
MESH = pl.DeviceIdType.MESH
T = 256
TN = 256
SA = 2048
DIRECT = 4
EARLY = 2
LAG_FWD = 3
LAG_DOWN = 4
SLOTS = 5
GELU_C = math.sqrt(2.0 / math.pi)


def gelu(p):
    return 0.5 * p * (1.0 + jnp.tanh(GELU_C * (p + 0.044715 * (p * p * p))))


def each(lo, hi, fn):
    def body(i, c):
        fn(i)
        return c

    lax.fori_loop(lo, hi, body, 0)


def program(diag, x, w1, w2, y, xg, hga, hgb, yp, wv, w2v, xv, hv, hba, hbb, yf, yin, yo,
            s_of, s_ov, s_pv, s_qr, s_pm, s_qm, s_rm, r_p, r_q, r_r, r_pm, r_qm, r_rm, s_xd, r_xd,
            s_wt, r_wt, s_wc, r_wc, s_l, s_hl, s_hf, r_hf, s_hm, r_hm, s_hw, r_hw, s_yf, r_yf, s_ld, s_yo):
    f32 = jnp.float32
    rows, kq = x.shape
    kh, fq = w1.shape
    nq = w2.shape[1]
    sb = fq - SA
    n = rows // T
    steps = 2 * n
    last = steps - 1
    row, co, ci = lax.axis_index("row"), lax.axis_index("co"), lax.axis_index("ci")
    vert, far, mate = {"row": 1 - row}, {"co": 1 - co}, {"ci": 1 - ci}
    corner = {"row": 1 - row, "co": 1 - co}
    mine = SA if diag else sb
    hg_mine, hg_far = (hga, hgb) if diag else (hgb, hga)
    hb_mine, hb_far = (hba, hbb) if diag else (hbb, hba)

    def rdma(src, dst, send, recv, dev):
        return pltpu.make_async_remote_copy(
            src_ref=src, dst_ref=dst, send_sem=send, recv_sem=recv, device_id=dev, device_id_type=MESH)

    def tok(j):
        return pl.ds(pl.multiple_of(j * T, T), T)

    def cols(t):
        return pl.ds(pl.multiple_of(t * TN, TN), TN)

    def own(j, send, recv, dev):
        return rdma(x.at[tok(j)], xg.at[row, co, ci, tok(j)], send.at[j], recv.at[j], dev)

    def own_far(j):
        return own(j, s_of, r_p, far)

    def own_vert(j):
        return own(j, s_ov, r_q, vert)

    def pass_on(r, c, j, send, recv, dev):
        blk = xg.at[r, c, ci, tok(j)]
        return rdma(blk, blk, send.at[j], recv.at[j], dev)

    def p_vert(j):
        return pass_on(row, 1 - co, j, s_pv, r_r, vert)

    def q_far(j):
        return pass_on(1 - row, co, j, s_qr, r_r, far)

    def r_vert(j):
        return pass_on(1 - row, 1 - co, j, s_qr, r_p, vert)

    def p_mate(j):
        return pass_on(row, 1 - co, j, s_pm, r_pm, mate)

    def q_mate(j):
        return pass_on(1 - row, co, j, s_qm, r_qm, mate)

    def r_mate(j):
        return pass_on(1 - row, 1 - co, j, s_rm, r_rm, mate)

    def got(recv, j):
        own(j, s_of, recv, far).wait_recv()

    xd = rdma(x, xg.at[row, co, ci], s_xd.at[0], r_xd.at[0], mate)

    w_cross = rdma(w1.at[:, SA:], wv.at[row, :, :sb], s_wc.at[0], r_wc.at[row], far if diag else corner)

    def w_tile(t):
        return rdma(w1.at[:, cols(t)], wv.at[row, :, cols(t)], s_wt.at[t], r_wt.at[t], vert)

    def w_in(k):
        return rdma(w1.at[:, SA:], wv.at[k, :, :sb], s_wc.at[0], r_wc.at[k], far)

    w2_in = pltpu.make_async_copy(w2, w2v, s_l.at[1])

    def h_src(i):
        return hv.at[lax.rem(i, SLOTS), :, :mine]

    def hf(i):
        return rdma(h_src(i), hg_mine.at[ci, tok(i)], s_hf.at[i], r_hf.at[i], far)

    def hm(i):
        return rdma(h_src(i), hg_mine.at[ci, tok(i)], s_hm.at[i], r_hm.at[i], mate)

    def hl(i):
        return pltpu.make_async_copy(h_src(i), hg_mine.at[ci, tok(i)], s_hl.at[lax.rem(i, SLOTS)])

    def hw(i):
        blk = hg_far.at[ci, tok(i)]
        return rdma(blk, blk, s_hw.at[i], r_hw.at[i], mate)

    def hf_got(i):
        blk = hg_far.at[ci, tok(i)]
        rdma(blk, blk, s_hw.at[i], r_hf.at[i], far).wait_recv()

    def yc(j):
        return rdma(yf.at[j], yp.at[tok(j)], s_yf.at[j], r_yf.at[j], vert)

    def y_out(j):
        s = lax.rem(j, 2)
        return pltpu.make_async_copy(yo.at[s], y.at[tok(j)], s_yo.at[s])

    def bring(j):
        def through():
            got(r_p, j)
            own_vert(j).start()
            p_vert(j).start()
            p_mate(j).start()

        if diag:
            through()
        else:
            pl.when(j < DIRECT)(through)

            @pl.when(j >= DIRECT)
            def _():
                own_vert(j).start()
                got(r_q, j)
                q_far(j).start()

    def meet(j):
        if diag:
            got(r_q, j)
        else:
            @pl.when(j < DIRECT)
            def _():
                got(r_q, j)
        got(r_r, j)
        if diag:
            @pl.when(j >= DIRECT)
            def _():
                r_vert(j).start()
        q_mate(j).start()
        r_mate(j).start()

    def own_loads(j, s):
        return (
            pltpu.make_async_copy(xg.at[row, 1 - co, :, tok(j)], xv.at[s, 1 - co], s_ld.at[3 * s]),
            pltpu.make_async_copy(xg.at[row, co, 1 - ci, tok(j)], xv.at[s, co, 1 - ci], s_ld.at[3 * s + 1]),
            pltpu.make_async_copy(x.at[tok(j)], xv.at[s, co, ci], s_ld.at[3 * s + 2]),
        )

    def up_tile(xs, hs, t):
        p = None
        for a in range(2):
            for b in range(2):
                d = jnp.dot(xv[xs, a, b], wv[a, b * kq:(b + 1) * kq, cols(t)], preferred_element_type=f32)
                p = d if p is None else p + d
        hv[hs, :, cols(t)] = gelu(p).astype(jnp.bfloat16)

    def send_h(k):
        hf(k).start()
        hm(k).start()
        hl(k).start()

    def up(k):
        other = k < EARLY + n

        @pl.when(other)
        def _():
            j = k - EARLY
            got(r_qm, j)
            got(r_rm, j)
            ld = pltpu.make_async_copy(xg.at[1 - row, :, :, tok(j)], xv.at[0], s_ld.at[0])
            ld.start()
            ld.wait()

        @pl.when(jnp.logical_not(other))
        def _():
            j = k - n
            got(r_pm, j)
            for c in own_loads(j, 0):
                c.start()
            for c in own_loads(j, 0):
                c.wait()

        @pl.when(k >= SLOTS)
        def _():
            hf(k - SLOTS).wait_send()
            hm(k - SLOTS).wait_send()

        hs = lax.rem(k, SLOTS)
        each(0, mine // TN, lambda t: up_tile(0, hs, t))
        send_h(k)

    def w2_rows(first, b):
        lo = b * fq + (0 if first else SA)
        size = SA if first else sb
        return pl.ds(lo if isinstance(lo, int) else pl.multiple_of(lo, TN), size)

    def out(j, part):
        @pl.when(j >= 2)
        def _():
            y_out(j - 2).wait()

        yo[lax.rem(j, 2)] = (part + yin[...]).astype(jnp.bfloat16)
        y_out(j).start()

    def part_in(j):
        yc(j).wait_recv()
        c = pltpu.make_async_copy(yp.at[tok(j)], yin, s_ld.at[6])
        c.start()
        c.wait()

    def down(i):
        hl(i).wait()
        hm_got(i)
        hw(i).wait_recv()
        lda = pltpu.make_async_copy(hga.at[:, tok(i)], hba, s_ld.at[7])
        ldb = pltpu.make_async_copy(hgb.at[:, tok(i)], hbb, s_ld.at[8])
        lda.start()
        ldb.start()
        other = (i >= EARLY) & (i < EARLY + n)
        late = i >= EARLY + n
        s = jnp.where(i < EARLY, n + i, jnp.where(other, i - EARLY, n + EARLY))

        @pl.when(late)
        def _():
            part_in(i - n)

        lda.wait()
        ldb.wait()

        def tile(t):
            p = None
            for first, hb in ((True, hba), (False, hbb)):
                for b in range(2):
                    d = jnp.dot(hb[b], w2v[w2_rows(first, b), cols(t)], preferred_element_type=f32)
                    p = d if p is None else p + d
            yf[s, :, cols(t)] = p

        each(0, nq // TN, tile)

        @pl.when(other)
        def _():
            yc(i - EARLY).start()

        @pl.when(late)
        def _():
            out(i - n, yf[n + EARLY])

    def hm_got(i):
        blk = hg_mine.at[ci, tok(i)]
        rdma(blk, blk, s_hw.at[i], r_hm.at[i], mate).wait_recv()

    if diag:
        each(0, EARLY, lambda j: own_far(j).start())
        w_cross.start()
        each(EARLY, DIRECT, lambda j: own_far(j).start())
        here = pltpu.make_async_copy(w1.at[:, :SA], wv.at[row], s_l.at[0])
        here.start()
    else:
        each(0, SA // TN, lambda t: w_tile(t).start())
        each(0, EARLY, lambda j: own_far(j).start())
        w_cross.start()
        each(EARLY, n, lambda j: own_far(j).start())
    xd.start()
    w2_in.start()
    each(0, EARLY, bring)
    xd.wait_recv()
    for j in range(EARLY):
        got(r_pm, j)
        for c in own_loads(j, j):
            c.start()
    for j in range(EARLY):
        for c in own_loads(j, j):
            c.wait()
    if diag:
        here.wait()
    else:
        w_in(0).wait_recv()
        w_in(1).wait_recv()

    def first_tiles(t):
        if diag:
            rdma(w1.at[:, cols(t)], wv.at[1 - row, :, cols(t)], s_wt.at[t], r_wt.at[t], vert).wait_recv()
        for j in range(EARLY):
            up_tile(j, j, t)

    each(0, mine // TN, first_tiles)
    each(0, EARLY, send_h)
    w2_in.wait()
    each(EARLY, 2 * EARLY, bring)
    meet(0)

    def step(k):
        @pl.when(k < steps)
        def _():
            up(k)

        each(jnp.minimum(n, 2 * k), jnp.minimum(n, 2 * k + 2), bring)

        @pl.when(k - 1 < n)
        def _():
            meet(k - 1)

        if not diag:
            @pl.when((k >= n - 2 + DIRECT) & (k < 2 * n - 2))
            def _():
                got(r_p, k - (n - 2))
                p_mate(k - (n - 2)).start()

        @pl.when((k >= n + EARLY) & (k < n + 2 * EARLY))
        def _():
            j = k - n - EARLY
            part_in(j)
            out(j, yf[n + j])

        @pl.when(k >= LAG_DOWN)
        def _():
            down(k - LAG_DOWN)

        @pl.when(k >= LAG_FWD)
        def _():
            hf_got(k - LAG_FWD)
            hw(k - LAG_FWD).start()

    each(EARLY, last + LAG_FWD, step)
    each(last - 1, last, down)

    def piece(src, dst):
        c = pltpu.make_async_copy(src, dst, s_ld.at[7])
        c.start()
        c.wait()

    hl(last).wait()
    hm_got(last)
    piece(hg_mine.at[:, tok(last)], hb_mine)
    part_in(n - 1)
    y_out(n - 3).wait()

    def near(t):
        p = yin[:, cols(t)]
        for b in range(2):
            p = p + jnp.dot(hb_mine[b], w2v[w2_rows(diag, b), cols(t)], preferred_element_type=f32)
        yin[:, cols(t)] = p

    each(0, nq // TN, near)
    hf_got(last)
    hw(last).start()
    piece(hg_far.at[ci, tok(last)], hb_far.at[ci])

    def away(t):
        yin[:, cols(t)] += jnp.dot(hb_far[ci], w2v[w2_rows(not diag, ci), cols(t)], preferred_element_type=f32)

    each(0, nq // TN, away)
    hw(last).wait_recv()
    piece(hg_far.at[1 - ci, tok(last)], hb_far.at[1 - ci])

    def final(t):
        d = jnp.dot(hb_far[1 - ci], w2v[w2_rows(not diag, 1 - ci), cols(t)], preferred_element_type=f32)
        yo[(n - 1) % 2, :, cols(t)] = (yin[:, cols(t)] + d).astype(jnp.bfloat16)

    each(0, nq // TN, final)
    y_out(n - 1).start()

    w_cross.wait_send()
    xd.wait_send()
    if not diag:
        each(0, SA // TN, lambda t: w_tile(t).wait_send())
    each(0, DIRECT if diag else n, lambda j: own_far(j).wait_send())
    each(0, n if diag else DIRECT, lambda j: p_vert(j).wait_send())
    each(DIRECT, n, lambda j: (r_vert(j) if diag else q_far(j)).wait_send())

    def sent_x(j):
        for c in (own_vert, p_mate, q_mate, r_mate, yc):
            c(j).wait_send()

    each(0, n, sent_x)
    each(0, steps, lambda i: hw(i).wait_send())

    def sent_h(i):
        hf(i).wait_send()
        hm(i).wait_send()

    each(steps - SLOTS, steps, sent_h)
    each(n - 2, n, lambda j: y_out(j).wait())


def kernel(*refs):
    row, co, ci = lax.axis_index("row"), lax.axis_index("co"), lax.axis_index("ci")
    barrier = pltpu.get_barrier_semaphore()
    for dev in ({"row": 1 - row}, {"co": 1 - co}, {"ci": 1 - ci}, {"row": 1 - row, "co": 1 - co}):
        pl.semaphore_signal(barrier, inc=1, device_id=dev, device_id_type=MESH)
    pl.semaphore_wait(barrier, 4)

    @pl.when(row == co)
    def _():
        program(True, *refs)

    @pl.when(row != co)
    def _():
        program(False, *refs)


def solution(mesh):
    def local_mlp(x, w1, w2):
        rows, kq = x.shape
        kh, fq = w1.shape
        fh, nq = w2.shape
        sb, n = fq - SA, rows // T
        bf, f32 = jnp.bfloat16, jnp.float32
        hbm = pl.BlockSpec(memory_space=pltpu.HBM)
        dma = lambda k: pltpu.SemaphoreType.DMA((k,))
        outs = pl.pallas_call(
            kernel,
            name="mlp",
            out_shape=(
                jax.ShapeDtypeStruct((rows, nq), bf),
                jax.ShapeDtypeStruct((2, 2, 2, rows, kq), bf),
                jax.ShapeDtypeStruct((2, 2 * rows, SA), bf),
                jax.ShapeDtypeStruct((2, 2 * rows, sb), bf),
                jax.ShapeDtypeStruct((rows, nq), f32),
            ),
            in_specs=[hbm] * 3,
            out_specs=(hbm,) * 5,
            scratch_shapes=[
                pltpu.VMEM((2, kh, SA), bf),
                pltpu.VMEM((fh, nq), bf),
                pltpu.VMEM((EARLY, 2, 2, T, kq), bf),
                pltpu.VMEM((SLOTS, T, SA), bf),
                pltpu.VMEM((2, T, SA), bf),
                pltpu.VMEM((2, T, sb), bf),
                pltpu.VMEM((n + EARLY + 1, T, nq), f32),
                pltpu.VMEM((T, nq), f32),
                pltpu.VMEM((2, T, nq), bf),
                *[dma(n)] * 13, dma(1), dma(1),
                dma(SA // TN), dma(SA // TN), dma(1), dma(2), dma(2), dma(SLOTS),
                *[dma(2 * n)] * 6,
                dma(n), dma(n), dma(9), dma(2),
            ],
            compiler_params=pltpu.CompilerParams(
                collective_id=0, has_side_effects=True, vmem_limit_bytes=67_000_000),
        )(x, w1, w2)
        return outs[0]

    act_spec = P(ROW_AXES, COL_AXES)
    wgt_spec = P("row", COL_AXES)
    return jax.shard_map(local_mlp, mesh=mesh, in_specs=(act_spec, wgt_spec, wgt_spec), out_specs=act_spec, check_vma=False)
```

```python
import math

import jax
import jax.numpy as jnp
from jax import lax
from jax.experimental import pallas as pl
from jax.experimental.pallas import tpu as pltpu
from jax.sharding import PartitionSpec as P

ROW_AXES = ("dp", "row")
COL_AXES = ("co", "ci")
MESH = pl.DeviceIdType.MESH
T = 256
TN = 256
SA = 2048
DIRECT = 4
EARLY = 2
Z = 1
LAG_FWD = 3
LAG_DOWN = 4
SLOTS = 5
GELU_C = math.sqrt(2.0 / math.pi)


def gelu(p):
    return 0.5 * p * (1.0 + jnp.tanh(GELU_C * (p + 0.044715 * (p * p * p))))


def each(lo, hi, fn):
    def body(i, c):
        fn(i)
        return c

    lax.fori_loop(lo, hi, body, 0)


def program(diag, x, w1, w2, y, xg, hga, hgb, yp, zp, wv, w2v, xv, hv, hba, hbb, yf, yin, yo, yz,
            s_of, s_ov, s_pv, s_qr, s_pm, s_qm, s_rm, r_p, r_q, r_r, r_pm, r_qm, r_rm, s_xd, r_xd,
            s_wt, r_wt, s_wc, r_wc, s_l, s_hl, s_hf, r_hf, s_hm, r_hm, s_hw, r_hw, s_yf, r_yf, s_z, r_zp, r_z, s_ld, s_yo):
    f32 = jnp.float32
    rows, kq = x.shape
    kh, fq = w1.shape
    nq = w2.shape[1]
    sb = fq - SA
    n = rows // T
    steps = 2 * n
    last = steps - 1
    row, co, ci = lax.axis_index("row"), lax.axis_index("co"), lax.axis_index("ci")
    vert, far, mate = {"row": 1 - row}, {"co": 1 - co}, {"ci": 1 - ci}
    corner = {"row": 1 - row, "co": 1 - co}
    mine = SA if diag else sb
    hg_mine, hg_far = (hga, hgb) if diag else (hgb, hga)
    hb_mine, hb_far = (hba, hbb) if diag else (hbb, hba)

    def rdma(src, dst, send, recv, dev):
        return pltpu.make_async_remote_copy(
            src_ref=src, dst_ref=dst, send_sem=send, recv_sem=recv, device_id=dev, device_id_type=MESH)

    def tok(j):
        return pl.ds(pl.multiple_of(j * T, T), T)

    def cols(t):
        return pl.ds(pl.multiple_of(t * TN, TN), TN)

    def own(j, send, recv, dev):
        return rdma(x.at[tok(j)], xg.at[row, co, ci, tok(j)], send.at[j], recv.at[j], dev)

    def own_far(j):
        return own(j, s_of, r_p, far)

    def own_vert(j):
        return own(j, s_ov, r_q, vert)

    def pass_on(r, c, j, send, recv, dev):
        blk = xg.at[r, c, ci, tok(j)]
        return rdma(blk, blk, send.at[j], recv.at[j], dev)

    def p_vert(j):
        return pass_on(row, 1 - co, j, s_pv, r_r, vert)

    def q_far(j):
        return pass_on(1 - row, co, j, s_qr, r_r, far)

    def r_vert(j):
        return pass_on(1 - row, 1 - co, j, s_qr, r_p, vert)

    def p_mate(j):
        return pass_on(row, 1 - co, j, s_pm, r_pm, mate)

    def q_mate(j):
        return pass_on(1 - row, co, j, s_qm, r_qm, mate)

    def r_mate(j):
        return pass_on(1 - row, 1 - co, j, s_rm, r_rm, mate)

    def got(recv, j):
        own(j, s_of, recv, far).wait_recv()

    xd = rdma(x, xg.at[row, co, ci], s_xd.at[0], r_xd.at[0], mate)

    w_cross = rdma(w1.at[:, SA:], wv.at[row, :, :sb], s_wc.at[0], r_wc.at[row], far if diag else corner)

    def w_tile(t):
        return rdma(w1.at[:, cols(t)], wv.at[row, :, cols(t)], s_wt.at[t], r_wt.at[t], vert)

    def w_in(k):
        return rdma(w1.at[:, SA:], wv.at[k, :, :sb], s_wc.at[0], r_wc.at[k], far)

    w2_in = pltpu.make_async_copy(w2, w2v, s_l.at[1])

    def h_src(i):
        return hv.at[lax.rem(i, SLOTS), :, :mine]

    def hf(i):
        return rdma(h_src(i), hg_mine.at[ci, tok(i)], s_hf.at[i], r_hf.at[i], far)

    def hm(i):
        return rdma(h_src(i), hg_mine.at[ci, tok(i)], s_hm.at[i], r_hm.at[i], mate)

    def hl(i):
        return pltpu.make_async_copy(h_src(i), hg_mine.at[ci, tok(i)], s_hl.at[lax.rem(i, SLOTS)])

    def hw(i):
        blk = hg_far.at[ci, tok(i)]
        return rdma(blk, blk, s_hw.at[i], r_hw.at[i], mate)

    def hf_got(i):
        blk = hg_far.at[ci, tok(i)]
        rdma(blk, blk, s_hw.at[i], r_hf.at[i], far).wait_recv()

    def yc(j):
        return rdma(yf.at[j], yp.at[tok(j)], s_yf.at[j], r_yf.at[j], vert)

    def z_part(j):
        return rdma(yf.at[n + j], zp.at[tok(j)], s_z.at[j], r_zp.at[j], vert)

    def z_sum(j):
        return rdma(yz.at[j], y.at[tok(j)], s_z.at[j], r_z.at[j], vert)

    def y_out(j):
        s = lax.rem(j, 2)
        return pltpu.make_async_copy(yo.at[s], y.at[tok(j)], s_yo.at[s])

    def bring(j):
        def through():
            got(r_p, j)
            own_vert(j).start()
            p_vert(j).start()
            p_mate(j).start()

        if diag:
            through()
        else:
            pl.when(j < DIRECT)(through)

            @pl.when(j >= DIRECT)
            def _():
                own_vert(j).start()
                got(r_q, j)
                q_far(j).start()

    def meet(j):
        if diag:
            got(r_q, j)
        else:
            @pl.when(j < DIRECT)
            def _():
                got(r_q, j)
        got(r_r, j)
        if diag:
            @pl.when(j >= DIRECT)
            def _():
                r_vert(j).start()
        q_mate(j).start()
        r_mate(j).start()

    def own_loads(j, s):
        return (
            pltpu.make_async_copy(xg.at[row, 1 - co, :, tok(j)], xv.at[s, 1 - co], s_ld.at[3 * s]),
            pltpu.make_async_copy(xg.at[row, co, 1 - ci, tok(j)], xv.at[s, co, 1 - ci], s_ld.at[3 * s + 1]),
            pltpu.make_async_copy(x.at[tok(j)], xv.at[s, co, ci], s_ld.at[3 * s + 2]),
        )

    def up_tile(xs, hs, t):
        p = None
        for a in range(2):
            for b in range(2):
                d = jnp.dot(xv[xs, a, b], wv[a, b * kq:(b + 1) * kq, cols(t)], preferred_element_type=f32)
                p = d if p is None else p + d
        hv[hs, :, cols(t)] = gelu(p).astype(jnp.bfloat16)

    def send_h(k):
        hf(k).start()
        hm(k).start()
        hl(k).start()

    def up(k):
        other = k < EARLY + n

        @pl.when(other)
        def _():
            j = k - EARLY
            got(r_qm, j)
            got(r_rm, j)
            ld = pltpu.make_async_copy(xg.at[1 - row, :, :, tok(j)], xv.at[0], s_ld.at[0])
            ld.start()
            ld.wait()

        @pl.when(jnp.logical_not(other))
        def _():
            j = k - n
            got(r_pm, j)
            for c in own_loads(j, 0):
                c.start()
            for c in own_loads(j, 0):
                c.wait()

        @pl.when(k >= SLOTS)
        def _():
            hf(k - SLOTS).wait_send()
            hm(k - SLOTS).wait_send()

        hs = lax.rem(k, SLOTS)
        each(0, mine // TN, lambda t: up_tile(0, hs, t))
        send_h(k)

    def w2_rows(first, b):
        lo = b * fq + (0 if first else SA)
        size = SA if first else sb
        return pl.ds(lo if isinstance(lo, int) else pl.multiple_of(lo, TN), size)

    def out(j, part):
        @pl.when(j >= 2 + (0 if diag else Z))
        def _():
            y_out(j - 2).wait()

        yo[lax.rem(j, 2)] = (part + yin[...]).astype(jnp.bfloat16)
        y_out(j).start()

    def part_in(j, copy=yc, ref=yp):
        copy(j).wait_recv()
        c = pltpu.make_async_copy(ref.at[tok(j)], yin, s_ld.at[6])
        c.start()
        c.wait()

    def down(i):
        hl(i).wait()
        hm_got(i)
        hw(i).wait_recv()
        lda = pltpu.make_async_copy(hga.at[:, tok(i)], hba, s_ld.at[7])
        ldb = pltpu.make_async_copy(hgb.at[:, tok(i)], hbb, s_ld.at[8])
        lda.start()
        ldb.start()
        other = (i >= EARLY) & (i < EARLY + n)
        late = i >= EARLY + n
        s = jnp.where(i < EARLY, n + i, jnp.where(other, i - EARLY, n + EARLY))

        @pl.when(late)
        def _():
            part_in(i - n)

        lda.wait()
        ldb.wait()

        def tile(t):
            p = None
            for first, hb in ((True, hba), (False, hbb)):
                for b in range(2):
                    d = jnp.dot(hb[b], w2v[w2_rows(first, b), cols(t)], preferred_element_type=f32)
                    p = d if p is None else p + d
            yf[s, :, cols(t)] = p

        each(0, nq // TN, tile)

        if not diag:
            @pl.when(i < Z)
            def _():
                z_part(i).start()

        @pl.when(other & (i >= EARLY + (Z if diag else 0)))
        def _():
            yc(i - EARLY).start()

        @pl.when(late)
        def _():
            out(i - n, yf[n + EARLY])

    def hm_got(i):
        blk = hg_mine.at[ci, tok(i)]
        rdma(blk, blk, s_hw.at[i], r_hm.at[i], mate).wait_recv()

    if diag:
        each(0, EARLY, lambda j: own_far(j).start())
        w_cross.start()
        each(EARLY, DIRECT, lambda j: own_far(j).start())
        here = pltpu.make_async_copy(w1.at[:, :SA], wv.at[row], s_l.at[0])
        here.start()
    else:
        each(0, SA // TN, lambda t: w_tile(t).start())
        each(0, EARLY, lambda j: own_far(j).start())
        w_cross.start()
        each(EARLY, n, lambda j: own_far(j).start())
    xd.start()
    w2_in.start()
    each(0, EARLY, bring)
    xd.wait_recv()
    for j in range(EARLY):
        got(r_pm, j)
        for c in own_loads(j, j):
            c.start()
    for j in range(EARLY):
        for c in own_loads(j, j):
            c.wait()
    if diag:
        here.wait()
    else:
        w_in(0).wait_recv()
        w_in(1).wait_recv()

    def first_tiles(t):
        if diag:
            rdma(w1.at[:, cols(t)], wv.at[1 - row, :, cols(t)], s_wt.at[t], r_wt.at[t], vert).wait_recv()
        for j in range(EARLY):
            up_tile(j, j, t)

    each(0, mine // TN, first_tiles)
    each(0, EARLY, send_h)
    w2_in.wait()
    each(EARLY, 2 * EARLY, bring)
    meet(0)

    def step(k):
        @pl.when(k < steps)
        def _():
            up(k)

        each(jnp.minimum(n, 2 * k), jnp.minimum(n, 2 * k + 2), bring)

        @pl.when(k - 1 < n)
        def _():
            meet(k - 1)

        if not diag:
            @pl.when((k >= n - 2 + DIRECT) & (k < 2 * n - 2))
            def _():
                got(r_p, k - (n - 2))
                p_mate(k - (n - 2)).start()

        @pl.when((k >= n + EARLY) & (k < n + 2 * EARLY))
        def _():
            j = k - n - EARLY

            def whole():
                part_in(j)
                out(j, yf[n + j])

            if diag:
                whole()

                @pl.when(j < Z)
                def _():
                    part_in(j, z_part, zp)
                    yz[j] = (yf[j] + yin[...]).astype(jnp.bfloat16)
                    z_sum(j).start()
            else:
                pl.when(j >= Z)(whole)

        @pl.when(k >= LAG_DOWN)
        def _():
            down(k - LAG_DOWN)

        @pl.when(k >= LAG_FWD)
        def _():
            hf_got(k - LAG_FWD)
            hw(k - LAG_FWD).start()

    each(EARLY, last + LAG_FWD, step)
    each(last - 1, last, down)

    def piece(src, dst):
        c = pltpu.make_async_copy(src, dst, s_ld.at[7])
        c.start()
        c.wait()

    hl(last).wait()
    hm_got(last)
    piece(hg_mine.at[:, tok(last)], hb_mine)
    y_out(n - 3).wait()

    def near(t):
        p = None
        for b in range(2):
            d = jnp.dot(hb_mine[b], w2v[w2_rows(diag, b), cols(t)], preferred_element_type=f32)
            p = d if p is None else p + d
        yf[n + EARLY, :, cols(t)] = p

    each(0, nq // TN, near)
    hf_got(last)
    hw(last).start()
    piece(hg_far.at[ci, tok(last)], hb_far.at[ci])

    def away(t):
        yf[n + EARLY, :, cols(t)] += jnp.dot(
            hb_far[ci], w2v[w2_rows(not diag, ci), cols(t)], preferred_element_type=f32)

    each(0, nq // TN, away)
    part_in(n - 1)
    hw(last).wait_recv()
    piece(hg_far.at[1 - ci, tok(last)], hb_far.at[1 - ci])

    def final(t):
        d = jnp.dot(hb_far[1 - ci], w2v[w2_rows(not diag, 1 - ci), cols(t)], preferred_element_type=f32)
        yo[(n - 1) % 2, :, cols(t)] = (yf[n + EARLY, :, cols(t)] + d + yin[:, cols(t)]).astype(jnp.bfloat16)

    each(0, nq // TN, final)
    y_out(n - 1).start()

    w_cross.wait_send()
    xd.wait_send()
    if not diag:
        each(0, SA // TN, lambda t: w_tile(t).wait_send())
    each(0, DIRECT if diag else n, lambda j: own_far(j).wait_send())
    each(0, n if diag else DIRECT, lambda j: p_vert(j).wait_send())
    each(DIRECT, n, lambda j: (r_vert(j) if diag else q_far(j)).wait_send())

    def sent_x(j):
        for c in (own_vert, p_mate, q_mate, r_mate):
            c(j).wait_send()

    each(0, n, sent_x)
    each(Z if diag else 0, n, lambda j: yc(j).wait_send())
    each(0, Z, lambda j: (z_sum if diag else z_part)(j).wait_send())
    if not diag:
        each(0, Z, lambda j: z_sum(j).wait_recv())
    each(0, steps, lambda i: hw(i).wait_send())

    def sent_h(i):
        hf(i).wait_send()
        hm(i).wait_send()

    each(steps - SLOTS, steps, sent_h)
    each(n - 2, n, lambda j: y_out(j).wait())


def kernel(*refs):
    row, co, ci = lax.axis_index("row"), lax.axis_index("co"), lax.axis_index("ci")
    barrier = pltpu.get_barrier_semaphore()
    for dev in ({"row": 1 - row}, {"co": 1 - co}, {"ci": 1 - ci}, {"row": 1 - row, "co": 1 - co}):
        pl.semaphore_signal(barrier, inc=1, device_id=dev, device_id_type=MESH)
    pl.semaphore_wait(barrier, 4)

    @pl.when(row == co)
    def _():
        program(True, *refs)

    @pl.when(row != co)
    def _():
        program(False, *refs)


def solution(mesh):
    def local_mlp(x, w1, w2):
        rows, kq = x.shape
        kh, fq = w1.shape
        fh, nq = w2.shape
        sb, n = fq - SA, rows // T
        bf, f32 = jnp.bfloat16, jnp.float32
        hbm = pl.BlockSpec(memory_space=pltpu.HBM)
        dma = lambda k: pltpu.SemaphoreType.DMA((k,))
        outs = pl.pallas_call(
            kernel,
            name="mlp",
            out_shape=(
                jax.ShapeDtypeStruct((rows, nq), bf),
                jax.ShapeDtypeStruct((2, 2, 2, rows, kq), bf),
                jax.ShapeDtypeStruct((2, 2 * rows, SA), bf),
                jax.ShapeDtypeStruct((2, 2 * rows, sb), bf),
                jax.ShapeDtypeStruct((rows, nq), f32),
                jax.ShapeDtypeStruct((Z * T, nq), f32),
            ),
            in_specs=[hbm] * 3,
            out_specs=(hbm,) * 6,
            scratch_shapes=[
                pltpu.VMEM((2, kh, SA), bf),
                pltpu.VMEM((fh, nq), bf),
                pltpu.VMEM((EARLY, 2, 2, T, kq), bf),
                pltpu.VMEM((SLOTS, T, SA), bf),
                pltpu.VMEM((2, T, SA), bf),
                pltpu.VMEM((2, T, sb), bf),
                pltpu.VMEM((n + EARLY + 1, T, nq), f32),
                pltpu.VMEM((T, nq), f32),
                pltpu.VMEM((2, T, nq), bf),
                pltpu.VMEM((Z, T, nq), bf),
                *[dma(n)] * 13, dma(1), dma(1),
                dma(SA // TN), dma(SA // TN), dma(1), dma(2), dma(2), dma(SLOTS),
                *[dma(2 * n)] * 6,
                dma(n), dma(n), dma(Z), dma(Z), dma(Z), dma(9), dma(2),
            ],
            compiler_params=pltpu.CompilerParams(
                collective_id=0, has_side_effects=True, vmem_limit_bytes=67_000_000),
        )(x, w1, w2)
        return outs[0]

    act_spec = P(ROW_AXES, COL_AXES)
    wgt_spec = P("row", COL_AXES)
    return jax.shard_map(local_mlp, mesh=mesh, in_specs=(act_spec, wgt_spec, wgt_spec), out_specs=act_spec, check_vma=False)
```

```python
import math

import jax
import jax.numpy as jnp
from jax import lax
from jax.experimental import pallas as pl
from jax.experimental.pallas import tpu as pltpu
from jax.sharding import PartitionSpec as P

ROW_AXES = ("dp", "row")
COL_AXES = ("co", "ci")
MESH = pl.DeviceIdType.MESH
T = 256
TN = 256
SA = 2048
DIRECT = 4
EARLY = 2
Z = 1
LAG_FWD = 3
LAG_DOWN = 4
SLOTS = 5
SUB = 2
HOLD = 6
GELU_C = math.sqrt(2.0 / math.pi)


def gelu(p):
    return 0.5 * p * (1.0 + jnp.tanh(GELU_C * (p + 0.044715 * (p * p * p))))


def each(lo, hi, fn):
    def body(i, c):
        fn(i)
        return c

    lax.fori_loop(lo, hi, body, 0)


def program(diag, x, w1, w2, y, xg, hga, hgb, yp, zp, wv, w2v, xv, hv, hba, hbb, hz, yf, yin, yo, yz,
            s_of, s_ov, s_pv, s_qr, s_pm, s_qm, s_rm, r_p, r_q, r_r, r_pm, r_qm, r_rm, s_xd, r_xd,
            s_wt, r_wt, s_wc, r_wc, s_l, s_hl, s_hf, r_hf, s_hm, r_hm, s_hw, r_hw, s_yf, r_yf, s_z, r_zp, r_z, s_hz, r_hz, s_hy, r_hy, s_yl, s_ld, s_yo):
    f32 = jnp.float32
    rows, kq = x.shape
    kh, fq = w1.shape
    nq = w2.shape[1]
    sb = fq - SA
    n = rows // T
    steps = 2 * n
    last = steps - 1
    row, co, ci = lax.axis_index("row"), lax.axis_index("co"), lax.axis_index("ci")
    vert, far, mate = {"row": 1 - row}, {"co": 1 - co}, {"ci": 1 - ci}
    corner = {"row": 1 - row, "co": 1 - co}
    mine = SA if diag else sb
    hg_mine, hg_far = (hga, hgb) if diag else (hgb, hga)
    hb_mine, hb_far = (hba, hbb) if diag else (hbb, hba)

    def rdma(src, dst, send, recv, dev):
        return pltpu.make_async_remote_copy(
            src_ref=src, dst_ref=dst, send_sem=send, recv_sem=recv, device_id=dev, device_id_type=MESH)

    def tok(j):
        return pl.ds(pl.multiple_of(j * T, T), T)

    def cols(t):
        return pl.ds(pl.multiple_of(t * TN, TN), TN)

    def own(j, send, recv, dev):
        return rdma(x.at[tok(j)], xg.at[row, co, ci, tok(j)], send.at[j], recv.at[j], dev)

    def own_far(j):
        return own(j, s_of, r_p, far)

    def own_vert(j):
        return own(j, s_ov, r_q, vert)

    def pass_on(r, c, j, send, recv, dev):
        blk = xg.at[r, c, ci, tok(j)]
        return rdma(blk, blk, send.at[j], recv.at[j], dev)

    def p_vert(j):
        return pass_on(row, 1 - co, j, s_pv, r_r, vert)

    def q_far(j):
        return pass_on(1 - row, co, j, s_qr, r_r, far)

    def r_vert(j):
        return pass_on(1 - row, 1 - co, j, s_qr, r_p, vert)

    def p_mate(j):
        return pass_on(row, 1 - co, j, s_pm, r_pm, mate)

    def q_mate(j):
        return pass_on(1 - row, co, j, s_qm, r_qm, mate)

    def r_mate(j):
        return pass_on(1 - row, 1 - co, j, s_rm, r_rm, mate)

    def got(recv, j):
        own(j, s_of, recv, far).wait_recv()

    xd = rdma(x, xg.at[row, co, ci], s_xd.at[0], r_xd.at[0], mate)

    w_cross = rdma(w1.at[:, SA:], wv.at[row, :, :sb], s_wc.at[0], r_wc.at[row], far if diag else corner)

    def w_tile(t):
        return rdma(w1.at[:, cols(t)], wv.at[row, :, cols(t)], s_wt.at[t], r_wt.at[t], vert)

    def w_in(k):
        return rdma(w1.at[:, SA:], wv.at[k, :, :sb], s_wc.at[0], r_wc.at[k], far)

    w2_in = pltpu.make_async_copy(w2, w2v, s_l.at[1])

    def h_src(i):
        return hv.at[lax.rem(i, SLOTS), :, :mine]

    def hf(i):
        return rdma(h_src(i), hg_mine.at[ci, tok(i)], s_hf.at[i], r_hf.at[i], far)

    def hm(i):
        return rdma(h_src(i), hg_mine.at[ci, tok(i)], s_hm.at[i], r_hm.at[i], mate)

    def hl(i):
        return pltpu.make_async_copy(h_src(i), hg_mine.at[ci, tok(i)], s_hl.at[lax.rem(i, SLOTS)])

    def hw(i):
        blk = hg_far.at[ci, tok(i)]
        return rdma(blk, blk, s_hw.at[i], r_hw.at[i], mate)

    def sub(u):
        return pl.ds(pl.multiple_of(u * (T // SUB), T // SUB), T // SUB)

    def hz_far(u):
        return rdma(hv.at[last % SLOTS, sub(u), :mine], hz.at[ci, sub(u), :mine], s_hz.at[u], r_hz.at[u], far)

    def hz_blk(c, u):
        return hz.at[c, sub(u), :fq - mine]

    def hz_got(u):
        rdma(hz_blk(ci, u), hz_blk(ci, u), s_hz.at[u], r_hz.at[u], far).wait_recv()

    def hz_mate(u):
        return rdma(hz_blk(ci, u), hz_blk(ci, u), s_hy.at[u], r_hy.at[u], mate)

    def hf_got(i):
        blk = hg_far.at[ci, tok(i)]
        rdma(blk, blk, s_hw.at[i], r_hf.at[i], far).wait_recv()

    def yc(j):
        return rdma(yf.at[j], yp.at[tok(j)], s_yf.at[j], r_yf.at[j], vert)

    def z_part(j):
        return rdma(yf.at[n + j], zp.at[tok(j)], s_z.at[j], r_zp.at[j], vert)

    def z_sum(j):
        return rdma(yz.at[j], y.at[tok(j)], s_z.at[j], r_z.at[j], vert)

    def y_out(j):
        s = lax.rem(j, 2)
        return pltpu.make_async_copy(yo.at[s], y.at[tok(j)], s_yo.at[s])

    def bring(j):
        def through():
            got(r_p, j)
            own_vert(j).start()
            p_vert(j).start()
            p_mate(j).start()

        if diag:
            through()
        else:
            pl.when(j < DIRECT)(through)

            @pl.when(j >= DIRECT)
            def _():
                own_vert(j).start()
                got(r_q, j)
                q_far(j).start()

    def meet(j):
        if diag:
            got(r_q, j)
        else:
            @pl.when(j < DIRECT)
            def _():
                got(r_q, j)
        got(r_r, j)
        if diag:
            @pl.when(j >= DIRECT)
            def _():
                r_vert(j).start()
        q_mate(j).start()
        r_mate(j).start()

    def own_loads(j, s):
        return (
            pltpu.make_async_copy(xg.at[row, 1 - co, :, tok(j)], xv.at[s, 1 - co], s_ld.at[3 * s]),
            pltpu.make_async_copy(xg.at[row, co, 1 - ci, tok(j)], xv.at[s, co, 1 - ci], s_ld.at[3 * s + 1]),
            pltpu.make_async_copy(x.at[tok(j)], xv.at[s, co, ci], s_ld.at[3 * s + 2]),
        )

    def up_tile(xs, hs, t):
        p = None
        for a in range(2):
            for b in range(2):
                d = jnp.dot(xv[xs, a, b], wv[a, b * kq:(b + 1) * kq, cols(t)], preferred_element_type=f32)
                p = d if p is None else p + d
        hv[hs, :, cols(t)] = gelu(p).astype(jnp.bfloat16)

    def send_h(k):
        @pl.when(k < last)
        def _():
            hf(k).start()

        @pl.when(k == last)
        def _():
            each(0, SUB, lambda u: hz_far(u).start())

        hm(k).start()
        hl(k).start()

    def up(k):
        other = k < EARLY + n

        @pl.when(other)
        def _():
            j = k - EARLY
            got(r_qm, j)
            got(r_rm, j)
            ld = pltpu.make_async_copy(xg.at[1 - row, :, :, tok(j)], xv.at[0], s_ld.at[0])
            ld.start()
            ld.wait()

        @pl.when(jnp.logical_not(other))
        def _():
            j = k - n
            got(r_pm, j)
            for c in own_loads(j, 0):
                c.start()
            for c in own_loads(j, 0):
                c.wait()

        @pl.when(k >= SLOTS)
        def _():
            hf(k - SLOTS).wait_send()
            hm(k - SLOTS).wait_send()

        hs = lax.rem(k, SLOTS)
        each(0, mine // TN, lambda t: up_tile(0, hs, t))
        send_h(k)

    def w2_rows(first, b):
        lo = b * fq + (0 if first else SA)
        size = SA if first else sb
        return pl.ds(lo if isinstance(lo, int) else pl.multiple_of(lo, TN), size)

    def out(j, part):
        @pl.when(j >= 2 + (0 if diag else Z))
        def _():
            y_out(j - 2).wait()

        yo[lax.rem(j, 2)] = (part + yin[...]).astype(jnp.bfloat16)
        y_out(j).start()

    def part_in(j, copy=yc, ref=yp):
        copy(j).wait_recv()
        c = pltpu.make_async_copy(ref.at[tok(j)], yin, s_ld.at[6])
        c.start()
        c.wait()

    def down(i):
        hl(i).wait()
        hm_got(i)
        hw(i).wait_recv()
        lda = pltpu.make_async_copy(hga.at[:, tok(i)], hba, s_ld.at[7])
        ldb = pltpu.make_async_copy(hgb.at[:, tok(i)], hbb, s_ld.at[8])
        lda.start()
        ldb.start()
        other = (i >= EARLY) & (i < EARLY + n)
        late = i >= EARLY + n
        s = jnp.where(i < EARLY, n + i, jnp.where(other, i - EARLY, n + EARLY))

        @pl.when(late)
        def _():
            part_in(i - n)

        lda.wait()
        ldb.wait()

        def tile(t):
            p = None
            for first, hb in ((True, hba), (False, hbb)):
                for b in range(2):
                    d = jnp.dot(hb[b], w2v[w2_rows(first, b), cols(t)], preferred_element_type=f32)
                    p = d if p is None else p + d
            yf[s, :, cols(t)] = p

        each(0, nq // TN, tile)

        if not diag:
            @pl.when(i < Z)
            def _():
                z_part(i).start()

        @pl.when(other & (i >= EARLY + (Z if diag else 0)))
        def _():
            yc(i - EARLY).start()

        @pl.when(late)
        def _():
            out(i - n, yf[n + EARLY])

    def hm_got(i):
        blk = hg_mine.at[ci, tok(i)]
        rdma(blk, blk, s_hw.at[i], r_hm.at[i], mate).wait_recv()

    if diag:
        each(0, EARLY, lambda j: own_far(j).start())
        w_cross.start()
        each(EARLY, DIRECT, lambda j: own_far(j).start())
        here = pltpu.make_async_copy(w1.at[:, :SA], wv.at[row], s_l.at[0])
        here.start()
    else:
        each(0, SA // TN, lambda t: w_tile(t).start())
        each(0, EARLY, lambda j: own_far(j).start())
        w_cross.start()
        each(EARLY, n, lambda j: own_far(j).start())
    xd.start()
    w2_in.start()
    if diag:
        each(0, EARLY, lambda j: own_vert(j).start())

        def near_only(j):
            got(r_p, j)
            p_mate(j).start()

        each(0, EARLY, near_only)
    else:
        each(0, EARLY, bring)
    xd.wait_recv()
    for j in range(EARLY):
        got(r_pm, j)
        for c in own_loads(j, j):
            c.start()
    for j in range(EARLY):
        for c in own_loads(j, j):
            c.wait()
    if diag:
        here.wait()
    else:
        w_in(0).wait_recv()
        w_in(1).wait_recv()

    def first_tiles(t):
        if diag:
            rdma(w1.at[:, cols(t)], wv.at[1 - row, :, cols(t)], s_wt.at[t], r_wt.at[t], vert).wait_recv()

            @pl.when(t == HOLD)
            def _():
                each(0, EARLY, lambda j: p_vert(j).start())

        for j in range(EARLY):
            up_tile(j, j, t)

    each(0, mine // TN, first_tiles)
    each(0, EARLY, send_h)
    w2_in.wait()
    each(EARLY, 2 * EARLY, bring)
    meet(0)

    def step(k):
        @pl.when(k < steps)
        def _():
            up(k)

        each(jnp.minimum(n, 2 * k), jnp.minimum(n, 2 * k + 2), bring)

        @pl.when(k - 1 < n)
        def _():
            meet(k - 1)

        if not diag:
            @pl.when((k >= n - 2 + DIRECT) & (k < 2 * n - 2))
            def _():
                got(r_p, k - (n - 2))
                p_mate(k - (n - 2)).start()

        @pl.when((k >= n + EARLY) & (k < n + 2 * EARLY))
        def _():
            j = k - n - EARLY

            def whole():
                part_in(j)
                out(j, yf[n + j])

            if diag:
                whole()

                @pl.when(j < Z)
                def _():
                    part_in(j, z_part, zp)
                    yz[j] = (yf[j] + yin[...]).astype(jnp.bfloat16)
                    z_sum(j).start()
            else:
                pl.when(j >= Z)(whole)

        @pl.when(k >= LAG_DOWN)
        def _():
            down(k - LAG_DOWN)

        @pl.when(k >= LAG_FWD)
        def _():
            hf_got(k - LAG_FWD)
            hw(k - LAG_FWD).start()

    each(EARLY, last + LAG_FWD, step)
    each(last - 1, last, down)

    def piece(src, dst):
        c = pltpu.make_async_copy(src, dst, s_ld.at[7])
        c.start()
        c.wait()

    hl(last).wait()
    hm_got(last)
    piece(hg_mine.at[:, tok(last)], hb_mine)
    y_out(n - 3).wait()

    def near(t):
        p = None
        for b in range(2):
            d = jnp.dot(hb_mine[b], w2v[w2_rows(diag, b), cols(t)], preferred_element_type=f32)
            p = d if p is None else p + d
        yf[n + EARLY, :, cols(t)] = p

    each(0, nq // TN, near)
    def y_last(u):
        s = (n - 1) % 2
        r = pl.ds(pl.multiple_of((n - 1) * T + u * (T // SUB), T // SUB), T // SUB)
        return pltpu.make_async_copy(yo.at[s, sub(u)], y.at[r], s_yl.at[u])

    def finish(u):
        hz_got(u)
        hz_mate(u).start()

        def away(t):
            yf[n + EARLY, sub(u), cols(t)] += jnp.dot(
                hz[ci, sub(u), :fq - mine], w2v[w2_rows(not diag, ci), cols(t)], preferred_element_type=f32)

        each(0, nq // TN, away)

        @pl.when(u == 0)
        def _():
            part_in(n - 1)

        hz_mate(u).wait_recv()

        def final(t):
            d = jnp.dot(hz[1 - ci, sub(u), :fq - mine], w2v[w2_rows(not diag, 1 - ci), cols(t)],
                        preferred_element_type=f32)
            yo[(n - 1) % 2, sub(u), cols(t)] = (
                yf[n + EARLY, sub(u), cols(t)] + d + yin[sub(u), cols(t)]).astype(jnp.bfloat16)

        each(0, nq // TN, final)
        y_last(u).start()

    each(0, SUB, finish)

    w_cross.wait_send()
    xd.wait_send()
    if not diag:
        each(0, SA // TN, lambda t: w_tile(t).wait_send())
    each(0, DIRECT if diag else n, lambda j: own_far(j).wait_send())
    each(0, n if diag else DIRECT, lambda j: p_vert(j).wait_send())
    each(DIRECT, n, lambda j: (r_vert(j) if diag else q_far(j)).wait_send())

    def sent_x(j):
        for c in (own_vert, p_mate, q_mate, r_mate):
            c(j).wait_send()

    each(0, n, sent_x)
    each(Z if diag else 0, n, lambda j: yc(j).wait_send())
    each(0, Z, lambda j: (z_sum if diag else z_part)(j).wait_send())
    if not diag:
        each(0, Z, lambda j: z_sum(j).wait_recv())
    each(0, last, lambda i: hw(i).wait_send())
    each(steps - SLOTS, last, lambda i: hf(i).wait_send())
    each(steps - SLOTS, steps, lambda i: hm(i).wait_send())

    def sent_last(u):
        hz_far(u).wait_send()
        hz_mate(u).wait_send()
        y_last(u).wait()

    each(0, SUB, sent_last)
    y_out(n - 2).wait()


def kernel(*refs):
    row, co, ci = lax.axis_index("row"), lax.axis_index("co"), lax.axis_index("ci")
    barrier = pltpu.get_barrier_semaphore()
    for dev in ({"row": 1 - row}, {"co": 1 - co}, {"ci": 1 - ci}, {"row": 1 - row, "co": 1 - co}):
        pl.semaphore_signal(barrier, inc=1, device_id=dev, device_id_type=MESH)
    pl.semaphore_wait(barrier, 4)

    @pl.when(row == co)
    def _():
        program(True, *refs)

    @pl.when(row != co)
    def _():
        program(False, *refs)


def solution(mesh):
    def local_mlp(x, w1, w2):
        rows, kq = x.shape
        kh, fq = w1.shape
        fh, nq = w2.shape
        sb, n = fq - SA, rows // T
        bf, f32 = jnp.bfloat16, jnp.float32
        hbm = pl.BlockSpec(memory_space=pltpu.HBM)
        dma = lambda k: pltpu.SemaphoreType.DMA((k,))
        outs = pl.pallas_call(
            kernel,
            name="mlp",
            out_shape=(
                jax.ShapeDtypeStruct((rows, nq), bf),
                jax.ShapeDtypeStruct((2, 2, 2, rows, kq), bf),
                jax.ShapeDtypeStruct((2, 2 * rows, SA), bf),
                jax.ShapeDtypeStruct((2, 2 * rows, sb), bf),
                jax.ShapeDtypeStruct((rows, nq), f32),
                jax.ShapeDtypeStruct((Z * T, nq), f32),
            ),
            in_specs=[hbm] * 3,
            out_specs=(hbm,) * 6,
            scratch_shapes=[
                pltpu.VMEM((2, kh, SA), bf),
                pltpu.VMEM((fh, nq), bf),
                pltpu.VMEM((EARLY, 2, 2, T, kq), bf),
                pltpu.VMEM((SLOTS, T, SA), bf),
                pltpu.VMEM((2, T, SA), bf),
                pltpu.VMEM((2, T, sb), bf),
                pltpu.VMEM((2, T, SA), bf),
                pltpu.VMEM((n + EARLY + 1, T, nq), f32),
                pltpu.VMEM((T, nq), f32),
                pltpu.VMEM((2, T, nq), bf),
                pltpu.VMEM((Z, T, nq), bf),
                *[dma(n)] * 13, dma(1), dma(1),
                dma(SA // TN), dma(SA // TN), dma(1), dma(2), dma(2), dma(SLOTS),
                *[dma(2 * n)] * 6,
                dma(n), dma(n), dma(Z), dma(Z), dma(Z), *[dma(SUB)] * 5, dma(9), dma(2),
            ],
            compiler_params=pltpu.CompilerParams(
                collective_id=0, has_side_effects=True, vmem_limit_bytes=67_000_000),
        )(x, w1, w2)
        return outs[0]

    act_spec = P(ROW_AXES, COL_AXES)
    wgt_spec = P("row", COL_AXES)
    return jax.shard_map(local_mlp, mesh=mesh, in_specs=(act_spec, wgt_spec, wgt_spec), out_specs=act_spec, check_vma=False)
```

```python
import math

import jax
import jax.numpy as jnp
from jax import lax
from jax.experimental import pallas as pl
from jax.experimental.pallas import tpu as pltpu
from jax.sharding import PartitionSpec as P

ROW_AXES = ("dp", "row")
COL_AXES = ("co", "ci")
MESH = pl.DeviceIdType.MESH
T = 256
TN = 256
SA = 2048
DIRECT = 4
EARLY = 2
Z = 1
LAG_FWD = 3
LAG_DOWN = 4
SLOTS = 5
SUB = 2
HOLD = 6
GELU_C = math.sqrt(2.0 / math.pi)


def gelu(p):
    return 0.5 * p * (1.0 + jnp.tanh(GELU_C * (p + 0.044715 * (p * p * p))))


def each(lo, hi, fn):
    def body(i, c):
        fn(i)
        return c

    lax.fori_loop(lo, hi, body, 0)


def program(diag, x, w1, w2, y, yl, xg, hga, hgb, yp, zp, wv, w2v, xv, hv, hba, hbb, hz, yf, yin, yo, yz,
            s_of, s_ov, s_pv, s_qr, s_pm, s_qm, s_rm, r_p, r_q, r_r, r_pm, r_qm, r_rm, s_xd, r_xd,
            s_wt, r_wt, s_wc, r_wc, s_l, s_hl, s_hf, r_hf, s_hm, r_hm, s_hw, r_hw, s_yf, r_yf, s_z, r_zp, r_z, s_hz, r_hz, s_hy, r_hy, s_yl, s_ld, s_yo):
    f32 = jnp.float32
    rows, kq = x.shape
    kh, fq = w1.shape
    nq = w2.shape[1]
    sb = fq - SA
    n = rows // T
    steps = 2 * n
    last = steps - 1
    row, co, ci = lax.axis_index("row"), lax.axis_index("co"), lax.axis_index("ci")
    vert, far, mate = {"row": 1 - row}, {"co": 1 - co}, {"ci": 1 - ci}
    corner = {"row": 1 - row, "co": 1 - co}
    mine = SA if diag else sb
    hg_mine, hg_far = (hga, hgb) if diag else (hgb, hga)
    hb_mine, hb_far = (hba, hbb) if diag else (hbb, hba)

    def rdma(src, dst, send, recv, dev):
        return pltpu.make_async_remote_copy(
            src_ref=src, dst_ref=dst, send_sem=send, recv_sem=recv, device_id=dev, device_id_type=MESH)

    def tok(j):
        return pl.ds(pl.multiple_of(j * T, T), T)

    def cols(t):
        return pl.ds(t * TN if isinstance(t, int) else pl.multiple_of(t * TN, TN), TN)

    def own(j, send, recv, dev):
        return rdma(x.at[tok(j)], xg.at[row, co, ci, tok(j)], send.at[j], recv.at[j], dev)

    def own_far(j):
        return own(j, s_of, r_p, far)

    def own_vert(j):
        return own(j, s_ov, r_q, vert)

    def pass_on(r, c, j, send, recv, dev):
        blk = xg.at[r, c, ci, tok(j)]
        return rdma(blk, blk, send.at[j], recv.at[j], dev)

    def p_vert(j):
        return pass_on(row, 1 - co, j, s_pv, r_r, vert)

    def q_far(j):
        return pass_on(1 - row, co, j, s_qr, r_r, far)

    def r_vert(j):
        return pass_on(1 - row, 1 - co, j, s_qr, r_p, vert)

    def p_mate(j):
        return pass_on(row, 1 - co, j, s_pm, r_pm, mate)

    def q_mate(j):
        return pass_on(1 - row, co, j, s_qm, r_qm, mate)

    def r_mate(j):
        return pass_on(1 - row, 1 - co, j, s_rm, r_rm, mate)

    def got(recv, j):
        own(j, s_of, recv, far).wait_recv()

    xd = rdma(x, xg.at[row, co, ci], s_xd.at[0], r_xd.at[0], mate)

    w_cross = rdma(w1.at[:, SA:], wv.at[row, :, :sb], s_wc.at[0], r_wc.at[row], far if diag else corner)

    def w_tile(t):
        return rdma(w1.at[:, cols(t)], wv.at[row, :, cols(t)], s_wt.at[t], r_wt.at[t], vert)

    def w_in(k):
        return rdma(w1.at[:, SA:], wv.at[k, :, :sb], s_wc.at[0], r_wc.at[k], far)

    w2_in = pltpu.make_async_copy(w2, w2v, s_l.at[1])

    def h_src(i):
        return hv.at[lax.rem(i, SLOTS), :, :mine]

    def hf(i):
        return rdma(h_src(i), hg_mine.at[ci, tok(i)], s_hf.at[i], r_hf.at[i], far)

    def hm(i):
        return rdma(h_src(i), hg_mine.at[ci, tok(i)], s_hm.at[i], r_hm.at[i], mate)

    def hl(i):
        return pltpu.make_async_copy(h_src(i), hg_mine.at[ci, tok(i)], s_hl.at[lax.rem(i, SLOTS)])

    def hw(i):
        blk = hg_far.at[ci, tok(i)]
        return rdma(blk, blk, s_hw.at[i], r_hw.at[i], mate)

    def sub(u):
        return pl.ds(pl.multiple_of(u * (T // SUB), T // SUB), T // SUB)

    def hz_far(u):
        return rdma(hv.at[last % SLOTS, sub(u), :mine], hz.at[ci, sub(u), :mine], s_hz.at[u], r_hz.at[u], far)

    def hz_blk(c, u):
        return hz.at[c, sub(u), :fq - mine]

    def hz_got(u):
        rdma(hz_blk(ci, u), hz_blk(ci, u), s_hz.at[u], r_hz.at[u], far).wait_recv()

    def hz_mate(u):
        return rdma(hz_blk(ci, u), hz_blk(ci, u), s_hy.at[u], r_hy.at[u], mate)

    def hf_got(i):
        blk = hg_far.at[ci, tok(i)]
        rdma(blk, blk, s_hw.at[i], r_hf.at[i], far).wait_recv()

    def yc(j):
        return rdma(yf.at[j], yp.at[tok(j)], s_yf.at[j], r_yf.at[j], vert)

    def z_part(j):
        return rdma(yf.at[n + j], zp.at[tok(j)], s_z.at[j], r_zp.at[j], vert)

    def z_sum(j):
        return rdma(yz.at[j], y.at[tok(j)], s_z.at[j], r_z.at[j], vert)

    def y_out(j):
        s = lax.rem(j, 2)
        return pltpu.make_async_copy(yo.at[s], y.at[tok(j)], s_yo.at[s])

    def bring(j):
        def through():
            got(r_p, j)
            own_vert(j).start()
            p_vert(j).start()
            p_mate(j).start()

        if diag:
            through()
        else:
            pl.when(j < DIRECT)(through)

            @pl.when(j >= DIRECT)
            def _():
                own_vert(j).start()
                got(r_q, j)
                q_far(j).start()

    def meet(j):
        if diag:
            got(r_q, j)
        else:
            @pl.when(j < DIRECT)
            def _():
                got(r_q, j)
        got(r_r, j)
        if diag:
            @pl.when(j >= DIRECT)
            def _():
                r_vert(j).start()
        q_mate(j).start()
        r_mate(j).start()

    def own_loads(j, s):
        return (
            pltpu.make_async_copy(xg.at[row, 1 - co, :, tok(j)], xv.at[s, 1 - co], s_ld.at[3 * s]),
            pltpu.make_async_copy(xg.at[row, co, 1 - ci, tok(j)], xv.at[s, co, 1 - ci], s_ld.at[3 * s + 1]),
            pltpu.make_async_copy(x.at[tok(j)], xv.at[s, co, ci], s_ld.at[3 * s + 2]),
        )

    def up_tile(xs, hs, t):
        p = None
        for a in range(2):
            for b in range(2):
                d = jnp.dot(xv[xs, a, b], wv[a, b * kq:(b + 1) * kq, cols(t)], preferred_element_type=f32)
                p = d if p is None else p + d
        hv[hs, :, cols(t)] = gelu(p).astype(jnp.bfloat16)

    def send_h(k):
        @pl.when(k < last)
        def _():
            hf(k).start()

        @pl.when(k == last)
        def _():
            each(0, SUB, lambda u: hz_far(u).start())

        hm(k).start()
        hl(k).start()

    def up(k):
        other = k < EARLY + n

        @pl.when(other)
        def _():
            j = k - EARLY
            got(r_qm, j)
            got(r_rm, j)
            ld = pltpu.make_async_copy(xg.at[1 - row, :, :, tok(j)], xv.at[0], s_ld.at[0])
            ld.start()
            ld.wait()

        @pl.when(jnp.logical_not(other))
        def _():
            j = k - n
            got(r_pm, j)
            for c in own_loads(j, 0):
                c.start()
            for c in own_loads(j, 0):
                c.wait()

        @pl.when(k >= SLOTS)
        def _():
            hf(k - SLOTS).wait_send()
            hm(k - SLOTS).wait_send()

        hs = lax.rem(k, SLOTS)
        each(0, mine // TN, lambda t: up_tile(0, hs, t))
        send_h(k)

    def w2_rows(first, b):
        lo = b * fq + (0 if first else SA)
        size = SA if first else sb
        return pl.ds(lo if isinstance(lo, int) else pl.multiple_of(lo, TN), size)

    def out(j, part):
        @pl.when(j >= 2 + (0 if diag else Z))
        def _():
            y_out(j - 2).wait()

        yo[lax.rem(j, 2)] = (part + yin[...]).astype(jnp.bfloat16)
        y_out(j).start()

    def part_in(j, copy=yc, ref=yp):
        copy(j).wait_recv()
        c = pltpu.make_async_copy(ref.at[tok(j)], yin, s_ld.at[6])
        c.start()
        c.wait()

    def down(i):
        hl(i).wait()
        hm_got(i)
        hw(i).wait_recv()
        lda = pltpu.make_async_copy(hga.at[:, tok(i)], hba, s_ld.at[7])
        ldb = pltpu.make_async_copy(hgb.at[:, tok(i)], hbb, s_ld.at[8])
        lda.start()
        ldb.start()
        other = (i >= EARLY) & (i < EARLY + n)
        late = i >= EARLY + n
        s = jnp.where(i < EARLY, n + i, jnp.where(other, i - EARLY, n + EARLY))

        @pl.when(late)
        def _():
            part_in(i - n)

        lda.wait()
        ldb.wait()

        def tile(t):
            p = None
            for first, hb in ((True, hba), (False, hbb)):
                for b in range(2):
                    d = jnp.dot(hb[b], w2v[w2_rows(first, b), cols(t)], preferred_element_type=f32)
                    p = d if p is None else p + d
            yf[s, :, cols(t)] = p

        each(0, nq // TN, tile)

        if not diag:
            @pl.when(i < Z)
            def _():
                z_part(i).start()

        @pl.when(other & (i >= EARLY + (Z if diag else 0)))
        def _():
            yc(i - EARLY).start()

        @pl.when(late)
        def _():
            out(i - n, yf[n + EARLY])

    def hm_got(i):
        blk = hg_mine.at[ci, tok(i)]
        rdma(blk, blk, s_hw.at[i], r_hm.at[i], mate).wait_recv()

    if diag:
        each(0, EARLY, lambda j: own_far(j).start())
        w_cross.start()
        each(EARLY, DIRECT, lambda j: own_far(j).start())
        here = pltpu.make_async_copy(w1.at[:, :SA], wv.at[row], s_l.at[0])
        here.start()
    else:
        each(0, EARLY, lambda j: own_far(j).start())
        w_cross.start()
        each(0, SA // TN, lambda t: w_tile(t).start())
        each(EARLY, n, lambda j: own_far(j).start())
    xd.start()
    w2_in.start()
    if diag:
        each(0, EARLY, lambda j: own_vert(j).start())

        def near_only(j):
            got(r_p, j)
            p_mate(j).start()

        each(0, EARLY, near_only)
    else:
        each(0, EARLY, bring)
    xd.wait_recv()
    for j in range(EARLY):
        got(r_pm, j)
        for c in own_loads(j, j):
            c.start()
    for j in range(EARLY):
        for c in own_loads(j, j):
            c.wait()
    if diag:
        here.wait()
    else:
        w_in(0).wait_recv()
        w_in(1).wait_recv()

    def first_tiles(t):
        if diag:
            rdma(w1.at[:, cols(t)], wv.at[1 - row, :, cols(t)], s_wt.at[t], r_wt.at[t], vert).wait_recv()

            @pl.when(t == HOLD)
            def _():
                each(0, EARLY, lambda j: p_vert(j).start())

        for j in range(EARLY):
            up_tile(j, j, t)

    each(0, mine // TN, first_tiles)
    each(0, EARLY, send_h)
    w2_in.wait()
    each(EARLY, 2 * EARLY, bring)
    meet(0)

    def step(k):
        @pl.when(k < steps)
        def _():
            up(k)

        each(jnp.minimum(n, 2 * k), jnp.minimum(n, 2 * k + 2), bring)

        @pl.when(k - 1 < n)
        def _():
            meet(k - 1)

        if not diag:
            @pl.when((k >= n - 2 + DIRECT) & (k < 2 * n - 2))
            def _():
                got(r_p, k - (n - 2))
                p_mate(k - (n - 2)).start()

        @pl.when((k >= n + EARLY) & (k < n + 2 * EARLY))
        def _():
            j = k - n - EARLY

            def whole():
                part_in(j)
                out(j, yf[n + j])

            if diag:
                whole()

                @pl.when(j < Z)
                def _():
                    part_in(j, z_part, zp)
                    yz[j] = (yf[j] + yin[...]).astype(jnp.bfloat16)
                    z_sum(j).start()
            else:
                pl.when(j >= Z)(whole)

        @pl.when(k >= LAG_DOWN)
        def _():
            down(k - LAG_DOWN)

        @pl.when(k >= LAG_FWD)
        def _():
            hf_got(k - LAG_FWD)
            hw(k - LAG_FWD).start()

    each(EARLY, last + LAG_FWD, step)
    each(last - 1, last, down)

    def piece(src, dst):
        c = pltpu.make_async_copy(src, dst, s_ld.at[7])
        c.start()
        c.wait()

    hl(last).wait()
    hm_got(last)
    piece(hg_mine.at[:, tok(last)], hb_mine)
    y_out(n - 3).wait()

    def near(t):
        p = None
        for b in range(2):
            d = jnp.dot(hb_mine[b], w2v[w2_rows(diag, b), cols(t)], preferred_element_type=f32)
            p = d if p is None else p + d
        yf[n + EARLY, :, cols(t)] = p

    each(0, nq // TN, near)
    def y_last(u):
        s = (n - 1) % 2
        return pltpu.make_async_copy(yo.at[s, sub(u)], yl.at[sub(u)], s_yl.at[u])

    def finish(u):
        hz_got(u)
        hz_mate(u).start()

        def away(t):
            yf[n + EARLY, sub(u), cols(t)] += jnp.dot(
                hz[ci, sub(u), :fq - mine], w2v[w2_rows(not diag, ci), cols(t)], preferred_element_type=f32)

        for t in range(nq // TN):
            away(t)

        @pl.when(u == 0)
        def _():
            part_in(n - 1)

        hz_mate(u).wait_recv()

        def final(t):
            d = jnp.dot(hz[1 - ci, sub(u), :fq - mine], w2v[w2_rows(not diag, 1 - ci), cols(t)],
                        preferred_element_type=f32)
            yo[(n - 1) % 2, sub(u), cols(t)] = (
                yf[n + EARLY, sub(u), cols(t)] + d + yin[sub(u), cols(t)]).astype(jnp.bfloat16)

        for t in range(nq // TN):
            final(t)
        y_last(u).start()

    each(0, SUB, finish)

    w_cross.wait_send()
    xd.wait_send()
    if not diag:
        each(0, SA // TN, lambda t: w_tile(t).wait_send())
    each(0, DIRECT if diag else n, lambda j: own_far(j).wait_send())
    each(0, n if diag else DIRECT, lambda j: p_vert(j).wait_send())
    each(DIRECT, n, lambda j: (r_vert(j) if diag else q_far(j)).wait_send())

    def sent_x(j):
        for c in (own_vert, p_mate, q_mate, r_mate):
            c(j).wait_send()

    each(0, n, sent_x)
    each(Z if diag else 0, n, lambda j: yc(j).wait_send())
    each(0, Z, lambda j: (z_sum if diag else z_part)(j).wait_send())
    if not diag:
        each(0, Z, lambda j: z_sum(j).wait_recv())
    each(0, last, lambda i: hw(i).wait_send())
    each(steps - SLOTS, last, lambda i: hf(i).wait_send())
    each(steps - SLOTS, steps, lambda i: hm(i).wait_send())

    def sent_last(u):
        hz_far(u).wait_send()
        hz_mate(u).wait_send()
        y_last(u).wait()

    each(0, SUB, sent_last)
    y_out(n - 2).wait()


def kernel(*refs):
    row, co, ci = lax.axis_index("row"), lax.axis_index("co"), lax.axis_index("ci")
    barrier = pltpu.get_barrier_semaphore()
    for dev in ({"row": 1 - row}, {"co": 1 - co}, {"ci": 1 - ci}, {"row": 1 - row, "co": 1 - co}):
        pl.semaphore_signal(barrier, inc=1, device_id=dev, device_id_type=MESH)
    pl.semaphore_wait(barrier, 4)

    @pl.when(row == co)
    def _():
        program(True, *refs)

    @pl.when(row != co)
    def _():
        program(False, *refs)


def solution(mesh):
    def local_mlp(x, w1, w2):
        rows, kq = x.shape
        kh, fq = w1.shape
        fh, nq = w2.shape
        sb, n = fq - SA, rows // T
        bf, f32 = jnp.bfloat16, jnp.float32
        hbm = pl.BlockSpec(memory_space=pltpu.HBM)
        dma = lambda k: pltpu.SemaphoreType.DMA((k,))
        outs = pl.pallas_call(
            kernel,
            name="mlp",
            out_shape=(
                jax.ShapeDtypeStruct((rows, nq), bf),
                jax.ShapeDtypeStruct((T, nq), bf),
                jax.ShapeDtypeStruct((2, 2, 2, rows, kq), bf),
                jax.ShapeDtypeStruct((2, 2 * rows, SA), bf),
                jax.ShapeDtypeStruct((2, 2 * rows, sb), bf),
                jax.ShapeDtypeStruct((rows, nq), f32),
                jax.ShapeDtypeStruct((Z * T, nq), f32),
            ),
            in_specs=[hbm] * 3,
            out_specs=(hbm,) * 7,
            scratch_shapes=[
                pltpu.VMEM((2, kh, SA), bf),
                pltpu.VMEM((fh, nq), bf),
                pltpu.VMEM((EARLY, 2, 2, T, kq), bf),
                pltpu.VMEM((SLOTS, T, SA), bf),
                pltpu.VMEM((2, T, SA), bf),
                pltpu.VMEM((2, T, sb), bf),
                pltpu.VMEM((2, T, SA), bf),
                pltpu.VMEM((n + EARLY + 1, T, nq), f32),
                pltpu.VMEM((T, nq), f32),
                pltpu.VMEM((2, T, nq), bf),
                pltpu.VMEM((Z, T, nq), bf),
                *[dma(n)] * 13, dma(1), dma(1),
                dma(SA // TN), dma(SA // TN), dma(1), dma(2), dma(2), dma(SLOTS),
                *[dma(2 * n)] * 6,
                dma(n), dma(n), dma(Z), dma(Z), dma(Z), *[dma(SUB)] * 5, dma(9), dma(2),
            ],
            compiler_params=pltpu.CompilerParams(
                collective_id=0, has_side_effects=True, vmem_limit_bytes=67_000_000),
        )(x, w1, w2)
        late = lax.broadcasted_iota(jnp.int32, (rows // T, T, nq), 0) == rows // T - 1
        return jnp.where(late, outs[1][None], outs[0].reshape(rows // T, T, nq)).reshape(rows, nq)

    act_spec = P(ROW_AXES, COL_AXES)
    wgt_spec = P("row", COL_AXES)
    return jax.shard_map(local_mlp, mesh=mesh, in_specs=(act_spec, wgt_spec, wgt_spec), out_specs=act_spec, check_vma=False)
```

```python
import math

import jax
import jax.numpy as jnp
from jax import lax
from jax.experimental import pallas as pl
from jax.experimental.pallas import tpu as pltpu
from jax.sharding import PartitionSpec as P

ROW_AXES = ("dp", "row")
COL_AXES = ("co", "ci")
MESH = pl.DeviceIdType.MESH
T = 256
TN = 256
SA = 2048
DIRECT = 4
EARLY = 2
Z = 1
LAG_FWD = 3
LAG_DOWN = 4
SLOTS = 5
SUB = 2
HOLD = 6
GELU_C = math.sqrt(2.0 / math.pi)


def gelu(p):
    return 0.5 * p * (1.0 + jnp.tanh(GELU_C * (p + 0.044715 * (p * p * p))))


def each(lo, hi, fn):
    def body(i, c):
        fn(i)
        return c

    lax.fori_loop(lo, hi, body, 0)


def program(diag, x, w1, w2, y, yl, xg, hga, hgb, yp, zp, wv, w2v, xv, hv, hba, hbb, hz, yf, yin, yo, yz,
            s_of, s_ov, s_pv, s_qr, s_pm, s_qm, s_rm, r_p, r_q, r_r, r_pm, r_qm, r_rm, s_xd, r_xd,
            s_wt, r_wt, s_wc, r_wc, s_l, s_hl, s_hf, r_hf, s_hm, r_hm, s_hw, r_hw, s_yf, r_yf, s_z, r_zp, r_z, s_hz, r_hz, s_hy, r_hy, s_yl, s_ld, s_yo):
    f32 = jnp.float32
    rows, kq = x.shape
    kh, fq = w1.shape
    nq = w2.shape[1]
    sb = fq - SA
    n = rows // T
    steps = 2 * n
    last = steps - 1
    row, co, ci = lax.axis_index("row"), lax.axis_index("co"), lax.axis_index("ci")
    vert, far, mate = {"row": 1 - row}, {"co": 1 - co}, {"ci": 1 - ci}
    corner = {"row": 1 - row, "co": 1 - co}
    mine = SA if diag else sb
    hg_mine, hg_far = (hga, hgb) if diag else (hgb, hga)
    hb_mine, hb_far = (hba, hbb) if diag else (hbb, hba)

    def rdma(src, dst, send, recv, dev):
        return pltpu.make_async_remote_copy(
            src_ref=src, dst_ref=dst, send_sem=send, recv_sem=recv, device_id=dev, device_id_type=MESH)

    def tok(j):
        return pl.ds(pl.multiple_of(j * T, T), T)

    def cols(t):
        return pl.ds(t * TN if isinstance(t, int) else pl.multiple_of(t * TN, TN), TN)

    def own(j, send, recv, dev):
        return rdma(x.at[tok(j)], xg.at[row, co, ci, tok(j)], send.at[j], recv.at[j], dev)

    def own_far(j):
        return own(j, s_of, r_p, far)

    def own_vert(j):
        return own(j, s_ov, r_q, vert)

    def pass_on(r, c, j, send, recv, dev):
        blk = xg.at[r, c, ci, tok(j)]
        return rdma(blk, blk, send.at[j], recv.at[j], dev)

    def p_vert(j):
        return pass_on(row, 1 - co, j, s_pv, r_r, vert)

    def q_far(j):
        return pass_on(1 - row, co, j, s_qr, r_r, far)

    def r_vert(j):
        return pass_on(1 - row, 1 - co, j, s_qr, r_p, vert)

    def p_mate(j):
        return pass_on(row, 1 - co, j, s_pm, r_pm, mate)

    def q_mate(j):
        return pass_on(1 - row, co, j, s_qm, r_qm, mate)

    def r_mate(j):
        return pass_on(1 - row, 1 - co, j, s_rm, r_rm, mate)

    def got(recv, j):
        own(j, s_of, recv, far).wait_recv()

    xd = rdma(x, xg.at[row, co, ci], s_xd.at[0], r_xd.at[0], mate)

    w_cross = rdma(w1.at[:, SA:], wv.at[row, :, :sb], s_wc.at[0], r_wc.at[row], far if diag else corner)

    def w_tile(t):
        return rdma(w1.at[:, cols(t)], wv.at[row, :, cols(t)], s_wt.at[t], r_wt.at[t], vert)

    def w_in(k):
        return rdma(w1.at[:, SA:], wv.at[k, :, :sb], s_wc.at[0], r_wc.at[k], far)

    w2_in = pltpu.make_async_copy(w2, w2v, s_l.at[1])

    def h_src(i):
        return hv.at[lax.rem(i, SLOTS), :, :mine]

    def hf(i):
        return rdma(h_src(i), hg_mine.at[ci, tok(i)], s_hf.at[i], r_hf.at[i], far)

    def hm(i):
        return rdma(h_src(i), hg_mine.at[ci, tok(i)], s_hm.at[i], r_hm.at[i], mate)

    def hl(i):
        return pltpu.make_async_copy(h_src(i), hg_mine.at[ci, tok(i)], s_hl.at[lax.rem(i, SLOTS)])

    def hw(i):
        blk = hg_far.at[ci, tok(i)]
        return rdma(blk, blk, s_hw.at[i], r_hw.at[i], mate)

    def sub(u):
        return pl.ds(pl.multiple_of(u * (T // SUB), T // SUB), T // SUB)

    def hz_far(u):
        return rdma(hv.at[last % SLOTS, sub(u), :mine], hz.at[ci, sub(u), :mine], s_hz.at[u], r_hz.at[u], far)

    def hz_blk(c, u):
        return hz.at[c, sub(u), :fq - mine]

    def hz_got(u):
        rdma(hz_blk(ci, u), hz_blk(ci, u), s_hz.at[u], r_hz.at[u], far).wait_recv()

    def hz_mate(u):
        return rdma(hz_blk(ci, u), hz_blk(ci, u), s_hy.at[u], r_hy.at[u], mate)

    def hf_got(i):
        blk = hg_far.at[ci, tok(i)]
        rdma(blk, blk, s_hw.at[i], r_hf.at[i], far).wait_recv()

    def yc(j):
        return rdma(yf.at[j], yp.at[tok(j)], s_yf.at[j], r_yf.at[j], vert)

    def z_part(j):
        return rdma(yf.at[n + j], zp.at[tok(j)], s_z.at[j], r_zp.at[j], vert)

    def z_sum(j):
        return rdma(yz.at[j], y.at[tok(j)], s_z.at[j], r_z.at[j], vert)

    def y_out(j):
        s = lax.rem(j, 2)
        return pltpu.make_async_copy(yo.at[s], y.at[tok(j)], s_yo.at[s])

    def bring(j):
        def through():
            got(r_p, j)
            own_vert(j).start()
            p_vert(j).start()
            p_mate(j).start()

        if diag:
            through()
        else:
            pl.when(j < DIRECT)(through)

            @pl.when(j >= DIRECT)
            def _():
                own_vert(j).start()
                got(r_q, j)
                q_far(j).start()

    def meet(j):
        if diag:
            got(r_q, j)
        else:
            @pl.when(j < DIRECT)
            def _():
                got(r_q, j)
        got(r_r, j)
        if diag:
            @pl.when(j >= DIRECT)
            def _():
                r_vert(j).start()
        q_mate(j).start()
        r_mate(j).start()

    def own_loads(j, s):
        return (
            pltpu.make_async_copy(xg.at[row, 1 - co, :, tok(j)], xv.at[s, 1 - co], s_ld.at[3 * s]),
            pltpu.make_async_copy(xg.at[row, co, 1 - ci, tok(j)], xv.at[s, co, 1 - ci], s_ld.at[3 * s + 1]),
            pltpu.make_async_copy(x.at[tok(j)], xv.at[s, co, ci], s_ld.at[3 * s + 2]),
        )

    def up_tile(xs, hs, t):
        p = None
        for a in range(2):
            for b in range(2):
                d = jnp.dot(xv[xs, a, b], wv[a, b * kq:(b + 1) * kq, cols(t)], preferred_element_type=f32)
                p = d if p is None else p + d
        hv[hs, :, cols(t)] = gelu(p).astype(jnp.bfloat16)

    def send_h(k):
        @pl.when(k < last)
        def _():
            hf(k).start()

        @pl.when(k == last)
        def _():
            each(0, SUB, lambda u: hz_far(u).start())

        hm(k).start()
        hl(k).start()

    def up(k):
        other = k < EARLY + n

        @pl.when(other)
        def _():
            j = k - EARLY
            got(r_qm, j)
            got(r_rm, j)
            ld = pltpu.make_async_copy(xg.at[1 - row, :, :, tok(j)], xv.at[0], s_ld.at[0])
            ld.start()
            ld.wait()

        @pl.when(jnp.logical_not(other))
        def _():
            j = k - n
            got(r_pm, j)
            for c in own_loads(j, 0):
                c.start()
            for c in own_loads(j, 0):
                c.wait()

        @pl.when(k >= SLOTS)
        def _():
            hf(k - SLOTS).wait_send()
            hm(k - SLOTS).wait_send()

        hs = lax.rem(k, SLOTS)
        each(0, mine // TN, lambda t: up_tile(0, hs, t))
        send_h(k)

    def w2_rows(first, b):
        lo = b * fq + (0 if first else SA)
        size = SA if first else sb
        return pl.ds(lo if isinstance(lo, int) else pl.multiple_of(lo, TN), size)

    def out(j, part):
        @pl.when(j >= 2 + (0 if diag else Z))
        def _():
            y_out(j - 2).wait()

        yo[lax.rem(j, 2)] = (part + yin[...]).astype(jnp.bfloat16)
        y_out(j).start()

    def part_in(j, copy=yc, ref=yp):
        copy(j).wait_recv()
        c = pltpu.make_async_copy(ref.at[tok(j)], yin, s_ld.at[6])
        c.start()
        c.wait()

    def down(i):
        hl(i).wait()
        hm_got(i)
        hw(i).wait_recv()
        lda = pltpu.make_async_copy(hga.at[:, tok(i)], hba, s_ld.at[7])
        ldb = pltpu.make_async_copy(hgb.at[:, tok(i)], hbb, s_ld.at[8])
        lda.start()
        ldb.start()
        other = (i >= EARLY) & (i < EARLY + n)
        late = i >= EARLY + n
        s = jnp.where(i < EARLY, n + i, jnp.where(other, i - EARLY, n + EARLY))

        @pl.when(late)
        def _():
            part_in(i - n)

        lda.wait()
        ldb.wait()

        def tile(t):
            p = None
            for first, hb in ((True, hba), (False, hbb)):
                for b in range(2):
                    d = jnp.dot(hb[b], w2v[w2_rows(first, b), cols(t)], preferred_element_type=f32)
                    p = d if p is None else p + d
            yf[s, :, cols(t)] = p

        each(0, nq // TN, tile)

        if not diag:
            @pl.when(i < Z)
            def _():
                z_part(i).start()

        @pl.when(other & (i >= EARLY + (Z if diag else 0)))
        def _():
            yc(i - EARLY).start()

        @pl.when(late)
        def _():
            out(i - n, yf[n + EARLY])

    def hm_got(i):
        blk = hg_mine.at[ci, tok(i)]
        rdma(blk, blk, s_hw.at[i], r_hm.at[i], mate).wait_recv()

    if diag:
        each(0, EARLY, lambda j: own_far(j).start())
        w_cross.start()
        each(EARLY, DIRECT, lambda j: own_far(j).start())
        here = pltpu.make_async_copy(w1.at[:, :SA], wv.at[row], s_l.at[0])
        here.start()
    else:
        each(0, EARLY, lambda j: own_far(j).start())
        w_cross.start()
        each(0, SA // TN, lambda t: w_tile(t).start())
        each(EARLY, n, lambda j: own_far(j).start())
    xd.start()
    w2_in.start()
    if diag:
        each(0, EARLY, lambda j: own_vert(j).start())

        def near_only(j):
            got(r_p, j)
            p_mate(j).start()

        each(0, EARLY, near_only)
    else:
        each(0, EARLY, bring)
    xd.wait_recv()
    for j in range(EARLY):
        got(r_pm, j)
        for c in own_loads(j, j):
            c.start()
    for j in range(EARLY):
        for c in own_loads(j, j):
            c.wait()
    if diag:
        here.wait()
    else:
        w_in(0).wait_recv()
        w_in(1).wait_recv()

    def first_tiles(t):
        if diag:
            rdma(w1.at[:, cols(t)], wv.at[1 - row, :, cols(t)], s_wt.at[t], r_wt.at[t], vert).wait_recv()

            @pl.when(t == HOLD)
            def _():
                each(0, EARLY, lambda j: p_vert(j).start())

        for j in range(EARLY):
            up_tile(j, j, t)

    each(0, mine // TN, first_tiles)
    each(0, EARLY, send_h)
    w2_in.wait()
    each(EARLY, 2 * EARLY, bring)
    meet(0)

    def step(k):
        @pl.when(k < steps)
        def _():
            up(k)

        each(jnp.minimum(n, 2 * k), jnp.minimum(n, 2 * k + 2), bring)

        @pl.when(k - 1 < n)
        def _():
            meet(k - 1)

        if not diag:
            @pl.when((k >= n - 2 + DIRECT) & (k < 2 * n - 2))
            def _():
                got(r_p, k - (n - 2))
                p_mate(k - (n - 2)).start()

        @pl.when((k >= n + EARLY) & (k < n + 2 * EARLY))
        def _():
            j = k - n - EARLY

            def whole():
                part_in(j)
                out(j, yf[n + j])

            if diag:
                whole()

                @pl.when(j < Z)
                def _():
                    part_in(j, z_part, zp)
                    yz[j] = (yf[j] + yin[...]).astype(jnp.bfloat16)
                    z_sum(j).start()
            else:
                pl.when(j >= Z)(whole)

        @pl.when(k >= LAG_DOWN)
        def _():
            down(k - LAG_DOWN)

        @pl.when(k >= LAG_FWD)
        def _():
            hf_got(k - LAG_FWD)
            hw(k - LAG_FWD).start()

    each(EARLY, last + LAG_FWD, step)
    each(last - 1, last, down)

    def piece(src, dst):
        c = pltpu.make_async_copy(src, dst, s_ld.at[7])
        c.start()
        c.wait()

    hl(last).wait()
    hm_got(last)
    piece(hg_mine.at[:, tok(last)], hb_mine)
    y_out(n - 3).wait()

    def near(t):
        p = None
        for b in range(2):
            d = jnp.dot(hb_mine[b], w2v[w2_rows(diag, b), cols(t)], preferred_element_type=f32)
            p = d if p is None else p + d
        yf[n + EARLY, :, cols(t)] = p

    each(0, nq // TN, near)
    def y_last(u):
        s = (n - 1) % 2
        return pltpu.make_async_copy(yo.at[s, sub(u)], yl.at[sub(u)], s_yl.at[u])

    def finish(u):
        hz_got(u)
        hz_mate(u).start()

        def away(t):
            yf[n + EARLY, sub(u), cols(t)] += jnp.dot(
                hz[ci, sub(u), :fq - mine], w2v[w2_rows(not diag, ci), cols(t)], preferred_element_type=f32)

        for t in range(nq // TN):
            away(t)

        @pl.when(u == 0)
        def _():
            part_in(n - 1)

        hz_mate(u).wait_recv()

        def final(t):
            d = jnp.dot(hz[1 - ci, sub(u), :fq - mine], w2v[w2_rows(not diag, 1 - ci), cols(t)],
                        preferred_element_type=f32)
            yo[(n - 1) % 2, sub(u), cols(t)] = (
                yf[n + EARLY, sub(u), cols(t)] + d + yin[sub(u), cols(t)]).astype(jnp.bfloat16)

        for t in range(nq // TN):
            final(t)
        y_last(u).start()

    w_cross.wait_send()
    xd.wait_send()
    if not diag:
        each(0, SA // TN, lambda t: w_tile(t).wait_send())
    each(0, DIRECT if diag else n, lambda j: own_far(j).wait_send())
    each(0, n if diag else DIRECT, lambda j: p_vert(j).wait_send())
    each(DIRECT, n, lambda j: (r_vert(j) if diag else q_far(j)).wait_send())

    def sent_x(j):
        for c in (own_vert, p_mate, q_mate, r_mate):
            c(j).wait_send()

    each(0, n, sent_x)
    each(Z if diag else 0, n - 1, lambda j: yc(j).wait_send())
    each(0, Z, lambda j: (z_sum if diag else z_part)(j).wait_send())
    if not diag:
        each(0, Z, lambda j: z_sum(j).wait_recv())
    each(0, last - 1, lambda i: hw(i).wait_send())
    each(steps - SLOTS, last - 1, lambda i: hf(i).wait_send())
    each(steps - SLOTS, last, lambda i: hm(i).wait_send())

    each(0, SUB, finish)
    yc(n - 1).wait_send()
    hw(last - 1).wait_send()
    hf(last - 1).wait_send()
    hm(last).wait_send()

    def sent_last(u):
        hz_far(u).wait_send()
        hz_mate(u).wait_send()
        y_last(u).wait()

    each(0, SUB, sent_last)
    y_out(n - 2).wait()


def kernel(*refs):
    row, co, ci = lax.axis_index("row"), lax.axis_index("co"), lax.axis_index("ci")
    barrier = pltpu.get_barrier_semaphore()
    for dev in ({"row": 1 - row}, {"co": 1 - co}, {"ci": 1 - ci}, {"row": 1 - row, "co": 1 - co}):
        pl.semaphore_signal(barrier, inc=1, device_id=dev, device_id_type=MESH)
    pl.semaphore_wait(barrier, 4)

    @pl.when(row == co)
    def _():
        program(True, *refs)

    @pl.when(row != co)
    def _():
        program(False, *refs)


def solution(mesh):
    def local_mlp(x, w1, w2):
        rows, kq = x.shape
        kh, fq = w1.shape
        fh, nq = w2.shape
        sb, n = fq - SA, rows // T
        bf, f32 = jnp.bfloat16, jnp.float32
        hbm = pl.BlockSpec(memory_space=pltpu.HBM)
        dma = lambda k: pltpu.SemaphoreType.DMA((k,))
        outs = pl.pallas_call(
            kernel,
            name="mlp",
            out_shape=(
                jax.ShapeDtypeStruct((rows, nq), bf),
                jax.ShapeDtypeStruct((T, nq), bf),
                jax.ShapeDtypeStruct((2, 2, 2, rows, kq), bf),
                jax.ShapeDtypeStruct((2, 2 * rows, SA), bf),
                jax.ShapeDtypeStruct((2, 2 * rows, sb), bf),
                jax.ShapeDtypeStruct((rows, nq), f32),
                jax.ShapeDtypeStruct((Z * T, nq), f32),
            ),
            in_specs=[hbm] * 3,
            out_specs=(hbm,) * 7,
            scratch_shapes=[
                pltpu.VMEM((2, kh, SA), bf),
                pltpu.VMEM((fh, nq), bf),
                pltpu.VMEM((EARLY, 2, 2, T, kq), bf),
                pltpu.VMEM((SLOTS, T, SA), bf),
                pltpu.VMEM((2, T, SA), bf),
                pltpu.VMEM((2, T, sb), bf),
                pltpu.VMEM((2, T, SA), bf),
                pltpu.VMEM((n + EARLY + 1, T, nq), f32),
                pltpu.VMEM((T, nq), f32),
                pltpu.VMEM((2, T, nq), bf),
                pltpu.VMEM((Z, T, nq), bf),
                *[dma(n)] * 13, dma(1), dma(1),
                dma(SA // TN), dma(SA // TN), dma(1), dma(2), dma(2), dma(SLOTS),
                *[dma(2 * n)] * 6,
                dma(n), dma(n), dma(Z), dma(Z), dma(Z), *[dma(SUB)] * 5, dma(9), dma(2),
            ],
            compiler_params=pltpu.CompilerParams(
                collective_id=0, has_side_effects=True, vmem_limit_bytes=67_000_000),
        )(x, w1, w2)
        late = lax.broadcasted_iota(jnp.int32, (rows // T, T, nq), 0) == rows // T - 1
        return jnp.where(late, outs[1][None], outs[0].reshape(rows // T, T, nq)).reshape(rows, nq)

    act_spec = P(ROW_AXES, COL_AXES)
    wgt_spec = P("row", COL_AXES)
    return jax.shard_map(local_mlp, mesh=mesh, in_specs=(act_spec, wgt_spec, wgt_spec), out_specs=act_spec, check_vma=False)
```
